32 devices in a mesh: dp: 4 (over x, core), mp: 8 (over z, y).
Axes of the slice: x: 2, y: 2, z: 4, core: 2. Of those that a mesh axis runs over, the one named last changes fastest.
Arguments:
- source_prompts: bfloat16 [128, 64, 4096], P(None, None, 'mp'), may hold values from -6 to 6
- task_logits: float32 [8, 128], replicated, may hold values from -8 to 260
- task_ids: int32 [32], P('dp'), may hold values from 0 to 7
- key_weight: bfloat16 [4096, 4096], P(None, 'mp'), may hold values from -0.09375 to 0.09375
- value_weight: bfloat16 [4096, 4096], P(None, 'mp'), may hold values from -0.09375 to 0.09375
- queries: bfloat16 [32, 128, 4096], P(('dp', 'mp')), may hold values from -32 to 32
- keys: bfloat16 [32, 128, 4096], P(('dp', 'mp')), may hold values from -16 to 16
- values: bfloat16 [32, 128, 4096], P(('dp', 'mp')), may hold values from -6 to 6
- cotangent: bfloat16 [32, 128, 4096], P(('dp', 'mp')), may hold values from -6 to 6
Outputs:
- attended: bfloat16 [32, 128, 4096], P(('dp', 'mp'))
- source_grad: float32 [128, 64, 4096], P(None, 'dp', 'mp')
- logits_grad: float32 [8, 128], replicated
The draws below stay inside these ranges and needn't reach their ends.
All inputs are finite; a program needn't handle non-finite values.
Results may differ from the reference program's by a relative error of at most 0.011.
Values may be sent and summed in bfloat16 or wider, within the bound.
A program may use at most 128 MiB of HBM per device.

```python
import jax
import jax.numpy as jnp
from jax import lax

D = 4096
HEADS = 32
DH = 128
NSRC = 128
NTASK = 8
PTOK = 64
SEQ = 128
EXAMPLES = 32


def query_key_pair(key):
    paired_key = jax.random.fold_in(key, 11)
    query_seed, key_seed = jax.random.split(paired_key, 2)
    full_shape = (EXAMPLES, SEQ, D)
    query_draw = jax.random.normal(query_seed, full_shape, jnp.float32)
    key_draw = jax.random.normal(key_seed, full_shape, jnp.float32)
    return (jnp.clip(query_draw, -32.0, 32.0), jnp.clip(key_draw, -16.0, 16.0))


def draw_queries(key, part):
    return query_key_pair(key)[0].astype(jnp.bfloat16)


def draw_keys(key, part):
    return query_key_pair(key)[1].astype(jnp.bfloat16)


def draw_task_logits(key, part):
    logit_key = jax.random.fold_in(key, 23)
    base_seed = jax.random.fold_in(logit_key, 0)
    logits = jnp.clip(2.0 * jax.random.normal(base_seed, (NTASK, NSRC), jnp.float32), -8.0, 8.0)
    return logits


def plant(result, own_key, smallest, high):
    place = [jax.random.randint(jax.random.fold_in(own_key, axis), (), 0, length) for axis, length in enumerate(result.shape)]
    main_axis = result.shape.index(max(result.shape))
    beside = place[:main_axis] + [(place[main_axis] + 1) % result.shape[main_axis]] + place[main_axis + 1:]
    return result.at[tuple(place)].set(smallest).at[tuple(beside)].set(high)


def steps_of(rng, extent, cuts, least, largest):
    level, own = 1.0, jax.random.fold_in(rng, 6)
    for dim, blocks in cuts:
        steps = jnp.exp(jax.random.uniform(jax.random.fold_in(own, dim), (blocks,), jnp.float32, least / len(cuts), largest / len(cuts)))
        level = level * jnp.repeat(steps, extent[dim] // blocks).reshape([-1 if axis == dim else 1 for axis in range(len(extent))])
    return level


def centred(own_key, shape, scale, limit, pieces=(), kind=jnp.bfloat16):
    loudness = steps_of(own_key, shape, pieces, -0.22, 0.18) if pieces else 1.0
    drawn = jax.random.normal(own_key, shape, jnp.float32) * scale * loudness
    return jnp.minimum(jnp.maximum(drawn, -limit), limit).astype(kind)


def setup_inputs(seed: int = 0) -> dict:
    streams_of = jax.random.split(jax.random.key(seed), 10)
    return {
        "source_prompts": centred(streams_of[0], (NSRC, PTOK, D), 1.0, 6.0, ((2, 8),)),
        "task_logits": draw_task_logits(jax.random.fold_in(streams_of[9], 71), 0),
        "task_ids": plant(jax.random.randint(streams_of[2], (EXAMPLES,), 0, NTASK), jax.random.fold_in(streams_of[2], 1), 0, NTASK - 1).astype(jnp.int32),
        "key_weight": centred(streams_of[3], (D, D), D ** -0.5, 0.09375, ((1, 8),)),
        "value_weight": centred(streams_of[4], (D, D), D ** -0.5, 0.09375, ((1, 8),)),
        "queries": draw_queries(jax.random.fold_in(streams_of[9], 71), 0),
        "keys": draw_keys(jax.random.fold_in(streams_of[9], 71), 0),
        "values": centred(streams_of[7], (EXAMPLES, SEQ, D), 1.0, 6.0, ((0, 32),)),
        "cotangent": centred(streams_of[8], (EXAMPLES, SEQ, D), 1.0, 6.0, ((0, 32),)),
    }


mask_fill = -1.0e30


def example_pass(prompt_pair, query_rows, key_rows, value_rows, cot_rows):
    score_scale = DH ** -0.5
    key_all = jnp.concatenate([prompt_pair[:, 0, :], key_rows], axis=0)
    value_all = jnp.concatenate([prompt_pair[:, 1, :], value_rows], axis=0)
    query_heads = query_rows.astype(jnp.float32).reshape(SEQ, HEADS, DH)
    key_heads = key_all.astype(jnp.float32).reshape(PTOK + SEQ, HEADS, DH)
    value_heads = value_all.astype(jnp.float32).reshape(PTOK + SEQ, HEADS, DH)
    cot_heads = cot_rows.astype(jnp.float32).reshape(SEQ, HEADS, DH)
    scores = jnp.einsum("ihd,jhd->hij", query_heads, key_heads) * score_scale
    column = jnp.arange(PTOK + SEQ)[None, :]
    position = jnp.arange(SEQ)[:, None]
    visible = (column < PTOK) | (column - PTOK <= position)
    scores = jnp.where(visible[None], scores, mask_fill)
    top_score = jnp.max(scores, axis=2, keepdims=True)
    exponent = jnp.exp(scores - top_score)
    attention = exponent / jnp.sum(exponent, axis=2, keepdims=True)
    attention_rounded = attention.astype(jnp.bfloat16)
    attended = jnp.einsum("hij,jhd->ihd", attention_rounded.astype(jnp.float32), value_heads)
    attended = attended.astype(jnp.bfloat16).reshape(SEQ, D)
    grad_attention = jnp.einsum("ihd,jhd->hij", cot_heads, value_heads)
    inner_sum = jnp.sum(attention * grad_attention, axis=2, keepdims=True)
    grad_scores = (attention * (grad_attention - inner_sum)).astype(jnp.bfloat16)
    key_grads = jnp.einsum("hij,ihd->jhd", grad_scores[:, :, :PTOK].astype(jnp.float32), query_heads)
    key_grads = (key_grads * score_scale).astype(jnp.bfloat16)
    value_grads = jnp.einsum("hij,ihd->jhd", attention_rounded[:, :, :PTOK].astype(jnp.float32), cot_heads)
    value_grads = value_grads.astype(jnp.bfloat16)
    return attended, jnp.stack([key_grads.reshape(PTOK, D), value_grads.reshape(PTOK, D)], axis=1)


def reference(source_prompts, task_logits, task_ids, key_weight, value_weight, queries, keys, values, cotangent):
    mix_weights = jax.nn.softmax(task_logits, axis=1)
    mix_rounded = mix_weights.astype(jnp.bfloat16)
    mixture = jnp.dot(mix_rounded, source_prompts.reshape(NSRC, PTOK * D), preferred_element_type=jnp.float32)
    mixture = mixture.astype(jnp.bfloat16).reshape(NTASK * PTOK, D)
    prompt_keys = jnp.dot(mixture, key_weight, preferred_element_type=jnp.float32).astype(jnp.bfloat16)
    prompt_values = jnp.dot(mixture, value_weight, preferred_element_type=jnp.float32).astype(jnp.bfloat16)
    prompt_table = jnp.stack([prompt_keys, prompt_values], axis=1).reshape(NTASK, PTOK, 2, D)

    def one_example(packed):
        task_index, query_rows, key_rows, value_rows, cot_rows = packed
        prompt_pair = lax.dynamic_index_in_dim(prompt_table, task_index, 0, keepdims=False)
        return example_pass(prompt_pair, query_rows, key_rows, value_rows, cot_rows)

    attended, prompt_grads = lax.map(one_example, (task_ids, queries, keys, values, cotangent))
    selector = (task_ids[:, None] == jnp.arange(NTASK, dtype=jnp.int32)[None, :]).astype(jnp.float32)
    task_grads = jnp.dot(selector.T, prompt_grads.reshape(EXAMPLES, PTOK * 2 * D).astype(jnp.float32),
                         precision=lax.Precision.HIGHEST)
    task_grads = task_grads.reshape(NTASK * PTOK, 2, D)
    mixture_grad = jnp.dot(task_grads[:, 0, :], key_weight.astype(jnp.float32).T, precision=lax.Precision.HIGHEST)
    mixture_grad = mixture_grad + jnp.dot(task_grads[:, 1, :], value_weight.astype(jnp.float32).T,
                                          precision=lax.Precision.HIGHEST)
    mixture_grad = mixture_grad.reshape(NTASK, PTOK * D)
    source_grad = jnp.dot(mix_weights.T, mixture_grad, precision=lax.Precision.HIGHEST).reshape(NSRC, PTOK, D)
    weight_grad = jnp.dot(mixture_grad, source_prompts.reshape(NSRC, PTOK * D).astype(jnp.float32).T,
                          precision=lax.Precision.HIGHEST)
    logits_grad = mix_weights * (weight_grad - jnp.sum(mix_weights * weight_grad, axis=1, keepdims=True))
    return attended, source_grad, logits_grad
```

```python
import functools

import jax
import jax.numpy as jnp
from jax import lax
from jax.experimental import pallas as pl
from jax.experimental.pallas import tpu as pltpu
from jax.sharding import PartitionSpec as P

D = 4096
HEADS = 32
DH = 128
NSRC = 128
NTASK = 8
PTOK = 64
SEQ = 128
E_DEV = 1


mask_fill = -1e30


def example_block(prompt_pair, queries, keys, values, cotangent):
    examples = queries.shape[0]
    score_scale = DH ** (-0.5)
    key_all = jnp.concatenate([prompt_pair[:, :, 0, :], keys], axis=1)
    value_all = jnp.concatenate([prompt_pair[:, :, 1, :], values], axis=1)
    query_heads = queries.reshape(examples, SEQ, HEADS, DH)
    key_heads = key_all.reshape(examples, PTOK + SEQ, HEADS, DH)
    value_heads = value_all.reshape(examples, PTOK + SEQ, HEADS, DH)
    cot_heads = cotangent.reshape(examples, SEQ, HEADS, DH)
    scores = (
        jnp.einsum("eihd,ejhd->ehij", query_heads, key_heads, preferred_element_type=jnp.float32)
        * score_scale
    )
    column = jnp.arange(PTOK + SEQ)[None, :]
    position = jnp.arange(SEQ)[:, None]
    visible = (column < PTOK) | (column - PTOK <= position)
    scores = jnp.where(visible[None, None], scores, mask_fill)
    top_score = jnp.max(scores, axis=3, keepdims=True)
    exponent = jnp.exp(scores - top_score)
    attention = exponent / jnp.sum(exponent, axis=3, keepdims=True)
    attention_rounded = attention.astype(jnp.bfloat16)
    attended = jnp.einsum(
        "ehij,ejhd->eihd", attention_rounded, value_heads, preferred_element_type=jnp.float32
    )
    attended = attended.astype(jnp.bfloat16).reshape(examples, SEQ, D)
    grad_attention = jnp.einsum(
        "eihd,ejhd->ehij", cot_heads, value_heads, preferred_element_type=jnp.float32
    )
    inner_sum = jnp.sum(attention * grad_attention, axis=3, keepdims=True)
    grad_scores = (attention * (grad_attention - inner_sum)).astype(jnp.bfloat16)
    key_grads = jnp.einsum(
        "ehij,eihd->ejhd",
        grad_scores[:, :, :, :PTOK],
        query_heads,
        preferred_element_type=jnp.float32,
    )
    key_grads = (key_grads * score_scale).astype(jnp.bfloat16).reshape(examples, PTOK, D)
    value_grads = jnp.einsum(
        "ehij,eihd->ejhd",
        attention_rounded[:, :, :, :PTOK],
        cot_heads,
        preferred_element_type=jnp.float32,
    )
    value_grads = value_grads.astype(jnp.bfloat16).reshape(examples, PTOK, D)
    return (attended, jnp.stack([key_grads, value_grads], axis=2))


def tile_products(tile_grad, source_prompts, mix_weights, col_width):
    rows_here = tile_grad.shape[1]
    own_prompts = lax.dynamic_slice_in_dim(
        source_prompts, lax.axis_index("dp") * rows_here, rows_here, 1
    )
    tile_flat = tile_grad.reshape(NTASK, rows_here * col_width)
    source_grad = jnp.dot(mix_weights.T, tile_flat, precision=lax.Precision.HIGHEST)
    source_grad = source_grad.reshape(NSRC, rows_here, col_width)
    weight_part = jnp.dot(
        tile_flat,
        own_prompts.reshape(NSRC, rows_here * col_width).astype(jnp.float32).T,
        precision=lax.Precision.HIGHEST,
    )
    return (source_grad, weight_part)


def on_device(
    source_prompts,
    task_logits,
    task_ids,
    key_weight,
    value_weight,
    queries,
    keys,
    values,
    cotangent,
):
    col_width = key_weight.shape[1]
    group_examples = task_ids.shape[0]
    mix_weights = jax.nn.softmax(task_logits, axis=1)
    mix_rounded = mix_weights.astype(jnp.bfloat16)
    mixture = jnp.dot(
        mix_rounded,
        source_prompts.reshape(NSRC, PTOK * col_width),
        preferred_element_type=jnp.float32,
    )
    mixture = mixture.astype(jnp.bfloat16).reshape(NTASK, PTOK, col_width)
    pair_weight = jnp.concatenate([key_weight, value_weight], axis=1)
    portion = lax.all_gather(mixture, "mp", axis=2, tiled=True)
    portion_rows = portion.reshape(NTASK * PTOK, portion.shape[2])
    projected = jnp.dot(portion_rows, pair_weight, preferred_element_type=jnp.float32)
    projected = projected.astype(jnp.bfloat16).reshape(NTASK, PTOK, 2, col_width)
    task_range = jnp.arange(NTASK, dtype=jnp.int32)
    selector_all = (task_ids[:, None] == task_range[None, :]).astype(jnp.bfloat16)
    table_full = lax.all_gather(projected, "mp", axis=3, tiled=True)
    own_offset = lax.axis_index("mp") * E_DEV
    own_selector = lax.dynamic_slice_in_dim(selector_all, own_offset, E_DEV, 0)
    chosen = jnp.dot(
        own_selector, table_full.reshape(NTASK, PTOK * 2 * D), preferred_element_type=jnp.float32
    )
    prompt_pair = chosen.astype(jnp.bfloat16).reshape(E_DEV, PTOK, 2, D)
    attended, outgoing_grads = example_block(prompt_pair, queries, keys, values, cotangent)
    incoming = lax.all_to_all(outgoing_grads, "mp", split_axis=3, concat_axis=0, tiled=True)
    group_grads = jnp.dot(
        selector_all.T,
        incoming.reshape(group_examples, PTOK * 2 * col_width),
        preferred_element_type=jnp.float32,
    )
    pair_weight_t = pair_weight.astype(jnp.float32).T
    task_rows = lax.psum_scatter(
        group_grads.reshape(NTASK, PTOK, 2 * col_width), "dp", scatter_dimension=1, tiled=True
    )
    rows_here = task_rows.shape[1]
    row_terms = jnp.dot(
        task_rows.reshape(NTASK * rows_here, 2 * col_width),
        pair_weight_t,
        precision=lax.Precision.HIGHEST,
    ).reshape(NTASK, rows_here, D)
    tile_grad = lax.psum_scatter(row_terms, "mp", scatter_dimension=2, tiled=True)
    source_grad, weight_part = tile_products(tile_grad, source_prompts, mix_weights, col_width)
    weight_grad = lax.psum(weight_part, ("dp", "mp"))
    logits_grad = mix_weights * (
        weight_grad - jnp.sum(mix_weights * weight_grad, axis=1, keepdims=True)
    )
    return (attended, source_grad, logits_grad)


BF = jnp.bfloat16
F32 = jnp.float32


def mm(a, b, ca=1, cb=0, precision=None):
    return lax.dot_general(
        a, b, (((ca,), (cb,)), ((), ())), preferred_element_type=F32, precision=precision
    )


def chain_kernel(
    ndp, nmp, nch,
    logits, ids_in, sp_hbm, kw_hbm, vw_hbm, q_hbm, k_hbm, v_hbm, c_hbm,
    att_hbm, tile_out, lg_out, w_hbm,
    att_out, w_out, p_v, kw_v, vw_v, q_v, k_v, v_v, c_v,
    mixed, ids_own, ids_buf, tab, sbuf, pair, gr, rbuf, acc, ubuf, urec, ys, yr, zs, zr, wp, wbuf,
    lsem, gs, gv, fs, fv, js, jv, ts, tv, bs, bv, cs, cv, us, uv, hs, hv, es, ev, ws, wv,
):
    n = ndp * nmp
    nz = nmp // 2
    ne = n // nz
    width = kw_v.shape[1]
    cw = width // nch
    rows = p_v.shape[1]
    nsrc = p_v.shape[0]
    ntask = logits.shape[0]
    tp = ntask * rows
    spn = nsrc * rows
    seq = q_v.shape[0]
    steps = nz * nch
    d = lax.axis_index("dp")
    m = lax.axis_index("mp")
    z = m // 2
    y = lax.rem(m, 2)
    me = d * nmp + m
    own = y * ndp + d
    up = 1 - 2 * (z // 2)
    inner = lax.rem((z + 1) // 2, 2)
    is_in = inner == 1
    nxt = z + up
    out_z = z - up * inner
    other = z * 2 + (1 - y)

    shift = rows.bit_length() - 1

    def iota(shape, axis):
        return lax.broadcasted_iota(jnp.int32, shape, axis)

    def outer(a):
        return lax.shift_right_logical(a, jnp.int32(shift))

    def same_row(shape):
        return ((iota(shape, 0) ^ iota(shape, 1)) & (rows - 1)) == 0

    def remote(src, dst, ss, rs, dd, mm_):
        return pltpu.make_async_remote_copy(
            src_ref=src, dst_ref=dst, send_sem=ss, recv_sem=rs,
            device_id=(dd, mm_), device_id_type=pl.DeviceIdType.MESH,
        )

    def place(i):
        i = jnp.int32(i)
        j = i - nch
        mid = 1 - 2 * lax.rem(jnp.maximum(j, 0), 2)
        off_in = jnp.where(i < nch, 0, jnp.where(i < 3 * nch, mid, 2))
        h_in = jnp.where(i < nch, i, jnp.where(i < 3 * nch, jnp.maximum(j, 0) // 2, i - 3 * nch))
        off = inner * off_in + (1 - inner) * (i // nch)
        return z + up * off, inner * h_in + (1 - inner) * lax.rem(i, nch)

    barrier = pltpu.get_barrier_semaphore()

    @pl.loop(1, n)
    def _(k):
        to = lax.rem(me + k, n)
        pl.semaphore_signal(
            barrier, inc=1, device_id=(to // nmp, lax.rem(to, nmp)),
            device_id_type=pl.DeviceIdType.MESH,
        )

    npl = 4
    loads = []
    for i in range(npl):
        s_at = pl.ds(i * (nsrc // npl), nsrc // npl)
        loads.append(
            pltpu.make_async_copy(
                sp_hbm.at[s_at, pl.ds(pl.multiple_of(d * rows, rows), rows), :],
                p_v.at[s_at], lsem.at[9 + i],
            )
        )
        loads[i].start()
    for i, (a, b) in enumerate(
        ((kw_hbm, kw_v), (vw_hbm, vw_v), (k_hbm, k_v), (q_hbm, q_v), (v_hbm, v_v), (c_hbm, c_v))
    ):
        loads.append(pltpu.make_async_copy(a, b, lsem.at[1 + i]))

    lg = logits[...]
    ex = jnp.exp(lg - jnp.max(lg, axis=1, keepdims=True))
    mix = ex / jnp.sum(ex, axis=1, keepdims=True)
    upm = (
        outer(iota((tp, ntask), 0)) == iota((tp, ntask), 1)
    )
    tall = mm(jnp.where(upm, 1.0, 0.0), mix.astype(BF).astype(F32)).astype(BF)
    out = (
        outer(iota((nsrc, spn), 1)) == iota((nsrc, spn), 0)
    )
    wide = mm(tall, jnp.where(out, 1.0, 0.0).astype(BF))
    w_out[...] = jnp.where(same_row((tp, spn)), wide, 0.0).astype(BF)
    for j in range(ids_in.shape[0]):
        line = jnp.full((1, tp), ids_in[j], jnp.int32).astype(F32)
        ids_own[pl.ds(j, 1), :] = line
        ids_buf[d, pl.ds(j, 1), :] = line

    for c in loads[:npl]:
        c.wait()
    for c in loads[npl:]:
        c.start()
    w_save = pltpu.make_async_copy(w_out, w_hbm, lsem.at[7])
    w_save.start()
    for h in range(nch):
        mixed[m, h] = mm(w_out[...], p_v[:, :, pl.ds(h * cw, cw)].reshape(spn, cw)).astype(BF)

    pl.semaphore_wait(barrier, n - 1)

    def g_copy(zz, h, dz):
        k = zz * nch + h
        slot = zz * 2 + y
        return remote(mixed.at[slot, h], mixed.at[slot, h], gs.at[k], gv.at[k], d, dz * 2 + y)

    def g2_copy(h):
        k = nz * nch + h
        slot = z * 2 + y
        return remote(
            mixed.at[slot, h], mixed.at[slot, h], gs.at[k], gv.at[z * nch + h], d, out_z * 2 + y
        )

    def f_copy(zz, h, yy):
        k = zz * nch + h
        slot = zz * 2 + yy
        return remote(mixed.at[slot, h], mixed.at[slot, h], fs.at[k], fv.at[k], d, other)

    for h in range(nch):
        g_copy(z, h, nxt).start()

        @pl.when(is_in)
        def _():
            g2_copy(h).start()

        f_copy(z, h, y).start()
    idc = []
    for j in range(1, ndp):
        c = remote(ids_own, ids_buf.at[d], js.at[j], jv.at[j], lax.rem(d + j, ndp), m)
        c.start()
        idc.append(c)
    loads[npl].wait()
    loads[npl + 1].wait()

    def part(slot, h):
        block = mixed[slot, h]
        at = pl.ds(pl.multiple_of(slot * width + h * cw, cw), cw)
        return mm(block, kw_v[at, :]), mm(block, vw_v[at, :])

    pk, pv = part(m, 0)
    for h in range(1, nch):
        a, b = part(m, h)
        pk, pv = pk + a, pv + b
    for i in range(nch, steps + nch):
        if i < steps:
            zz, h = place(i)
            g_copy(zz, h, nxt).wait_recv()

            @pl.when(is_in)
            def _():
                far = jnp.where(zz == out_z, nxt, out_z)
                g_copy(zz, h, far).start()

            f_copy(zz, h, y).start()
            a, b = part(zz * 2 + y, h)
            pk, pv = pk + a, pv + b
        zz, h = place(i - nch)
        f_copy(zz, h, 1 - y).wait_recv()
        a, b = part(zz * 2 + (1 - y), h)
        pk, pv = pk + a, pv + b
    for h in range(nch):
        at = slice(h * cw, (h + 1) * cw)
        tab[z * nch + h, :, :cw] = pk[:, at].astype(BF)
        tab[z * nch + h, :, cw:] = pv[:, at].astype(BF)
    for c in idc:
        c.wait()

    ids_all = ids_buf[...].reshape(n, tp).astype(BF)
    q_rows = 2 * ne * rows
    q = outer(iota((q_rows, n), 0))
    q_z = jnp.where(q < ne, z, out_z)
    q_in = q & (ne - 1)
    q_dev = lax.rem(q_in, jnp.int32(ndp)) * nmp + q_z * 2 + q_in // jnp.int32(ndp)
    ids_x = mm(jnp.where(q_dev == iota((q_rows, n), 1), 1.0, 0.0).astype(BF), ids_all)
    sel = jnp.where(
        (ids_x == outer(iota((q_rows, tp), 1)).astype(F32)) & same_row((q_rows, tp)), 1.0, 0.0
    ).astype(BF)
    sel_own = sel[: ne * rows]

    def row_at(dd):
        return pl.ds(pl.multiple_of(dd * rows, rows), rows)

    def col_at(zz, yy, h):
        return pl.ds(pl.multiple_of((zz * 2 + yy) * width + h * cw, cw), cw)

    def t_copy(zz, h):
        k = zz * nch + h
        return remote(tab.at[k], tab.at[k], ts.at[k], tv.at[k], d, nxt * 2 + y)

    def b_copy(zz, h, e, to_out):
        k = zz * nch + h
        g = e + to_out * ne
        return remote(
            sbuf.at[k, g], pair.at[:, row_at(d), col_at(zz, y, h)],
            bs.at[k * 2 * ne + g], bv.at[k * ne + own],
            lax.rem(e, ndp), (out_z if to_out else z) * 2 + e // ndp,
        )

    def b_wait(zz, h, e):
        k = zz * nch + h
        remote(
            sbuf.at[k, e], pair.at[:, row_at(lax.rem(e, ndp)), col_at(zz, e // ndp, h)],
            bs.at[k * 2 * ne + e], bv.at[k * ne + e], d, other,
        ).wait_recv()

    def relay(i):
        zz, h = place(i)
        k = zz * nch + h

        @pl.when(zz != z)
        def _():
            t_copy(zz, h).wait_recv()

        @pl.when((zz == z) | (zz == out_z))
        def _():
            t_copy(zz, h).start()

        got = mm(sel, tab[k]).astype(BF)
        sbuf[k, :, 0] = got[:, :cw].reshape(2 * ne, rows, cw)
        sbuf[k, :, 1] = got[:, cw:].reshape(2 * ne, rows, cw)

        @pl.when(is_in & (zz != out_z))
        def _():
            @pl.loop(0, ne)
            def _(r):
                b_copy(zz, h, lax.rem(own + r, ne), 1).start()

        @pl.loop(1, ne)
        def _(r):
            b_copy(zz, h, lax.rem(own + r, ne), 0).start()

        pair[:, row_at(d), col_at(zz, y, h)] = sbuf[k, own]

    for i in range(nch):
        relay(i)

    for c in loads[npl + 2:]:
        c.wait()

    def c_copy(zz, h, e):
        k = zz * nch + h
        return remote(
            gr.at[:, row_at(lax.rem(e, ndp)), col_at(zz, e // ndp, h)], rbuf.at[k, own],
            cs.at[k * ne + e], cv.at[k * ne + own], lax.rem(e, ndp), z * 2 + e // ndp,
        )

    def c_wait(zz, h, e):
        k = zz * nch + h
        remote(
            gr.at[:, row_at(lax.rem(e, ndp)), col_at(zz, e // ndp, h)], rbuf.at[k, e],
            cs.at[k * ne + e], cv.at[k * ne + e], d, other,
        ).wait_recv()

    scale = DH ** (-0.5)
    to_exp2 = scale * 1.4426950408889634
    ptok = pair.shape[1]
    seen = iota((seq, seq), 0) <= iota((seq, seq), 1)

    def group(i):
        zz, h = place(i)

        @pl.when(is_in | (zz == z))
        def _():
            @pl.loop(1, ne)
            def _(r):
                b_wait(zz, h, lax.rem(own + r, ne))

        @pl.when(jnp.logical_not(is_in | (zz == z)))
        def _():
            @pl.loop(0, ne)
            def _(r):
                b_wait(zz, h, r)

        ats, st, gt, va = [], [], [], []
        for yy in range(2):
            for hh in range(cw // DH):
                base = (zz * 2 + yy) * width + h * cw + hh * DH
                at = pl.ds(pl.multiple_of(base, DH), DH)
                ats.append(at)
                ka = jnp.concatenate([pair[0, :, at], k_v[:, at]], axis=0)
                va.append(jnp.concatenate([pair[1, :, at], v_v[:, at]], axis=0))
                st.append(mm(ka, q_v[:, at], 1, 1))
                gt.append(mm(va[-1], c_v[:, at], 1, 1))
        for j, at in enumerate(ats):
            s = st[j] * to_exp2
            s = jnp.concatenate([s[:ptok], jnp.where(seen, s[ptok:], mask_fill)], axis=0)
            e = jnp.exp2(s - jnp.max(s, axis=0, keepdims=True))
            a = e * (1.0 / jnp.sum(e, axis=0, keepdims=True))
            ab = a.astype(BF)
            inner_sum = jnp.sum(a * gt[j], axis=0, keepdims=True)
            gs1 = (a[:ptok] * (gt[j][:ptok] - inner_sum)).astype(BF)
            gr[0, :, at] = (mm(gs1, q_v[:, at]) * scale).astype(BF)
            gr[1, :, at] = mm(ab[:ptok], c_v[:, at]).astype(BF)
            att_out[:, at] = mm(ab, va[j], 0, 0).astype(BF)

        @pl.loop(1, ne)
        def _(r):
            c_copy(zz, h, lax.rem(own + r, ne)).start()

        rbuf[zz * nch + h, own] = gr[:, row_at(d), col_at(zz, y, h)]

    def u_copy(zz, h, dz, slot):
        k = zz * nch + h
        return remote(
            ubuf.at[k], urec.at[slot * nch + h], us.at[k], uv.at[slot * nch + h], d, dz * 2 + y
        )

    def total(i):
        zz, h = place(i)
        k = zz * nch + h

        @pl.loop(1, ne)
        def _(r):
            c_wait(zz, h, lax.rem(own + r, ne))

        acc[k, :, :cw] = mm(sel_own, rbuf[k, :, 0].reshape(ne * rows, cw), 0, 0)
        acc[k, :, cw:] = mm(sel_own, rbuf[k, :, 1].reshape(ne * rows, cw), 0, 0)

        @pl.when(is_in & (zz == out_z))
        def _():
            ubuf[k] = acc[k].astype(BF)
            u_copy(zz, h, out_z, z).start()

        @pl.when(jnp.logical_not(is_in | (zz == z)))
        def _():
            ubuf[k] = acc[k].astype(BF)
            u_copy(zz, h, nxt, zz).start()

    @pl.loop(0, steps)
    def _(i):
        @pl.when(is_in & (i < steps - nch))
        def _():
            relay(i + nch)

        group(i)

        @pl.when(i >= nch)
        def _():
            total(i - nch)

    att_save = pltpu.make_async_copy(att_out, att_hbm, lsem.at[8])
    att_save.start()

    @pl.loop(steps - nch, steps)
    def _(i):
        total(i)

    far = ((1, z + 2 * up), (2, z))

    def u_far(off, slot, h):
        return u_copy(z + up * off, h, z + up * off, slot)

    @pl.when(is_in)
    def _():
        for off, slot in far:
            for h in range(nch):
                zz = z + up * off
                k = zz * nch + h
                u_copy(zz, h, zz, zz).wait_recv()
                ubuf[k] = (acc[k] + urec[k].astype(F32)).astype(BF)
                u_far(off, slot, h).start()

    s1 = z + up * (1 - inner)
    s2 = z + up * (2 - 3 * inner)
    tks, tvs = [], []
    for h in range(nch):
        u_copy(z, h, nxt, s1).wait_recv()
        u_copy(z, h, nxt, s2).wait_recv()
        t = acc[z * nch + h] + urec[s1 * nch + h].astype(F32) + urec[s2 * nch + h].astype(F32)
        t = t.astype(BF)
        tks.append(t[:, :cw])
        tvs.append(t[:, cw:])
    tk = jnp.concatenate(tks, axis=1)
    tv_ = jnp.concatenate(tvs, axis=1)

    def term(slot, h):
        at = pl.ds(pl.multiple_of(slot * width + h * cw, cw), cw)
        return mm(tk, kw_v[at, :], 1, 1) + mm(tv_, vw_v[at, :], 1, 1)

    def target(j):
        return z + up * ((nz - 1 - j) * (1 - inner) + inner * (2, 1, -1, 0)[j])

    def y_copy(j, h):
        k = j * nch + h
        return remote(ys.at[k], yr.at[k], hs.at[k], hv.at[k], d, other)

    def z_copy(zz, h, dz, slot):
        k = zz * nch + h
        return remote(
            zs.at[k], zr.at[slot * nch + h], es.at[k], ev.at[slot * nch + h], d, dz * 2 + y
        )

    for j in range(nz):
        for h in range(nch):
            ys[j * nch + h] = term(target(j) * 2 + (1 - y), h).astype(BF)
            y_copy(j, h).start()

    def route(j):
        zz = target(j)
        if j == 0:
            return jnp.where(is_in, zz, nxt), jnp.where(is_in, z, zz)
        if j == 1:
            return jnp.where(is_in, zz, nxt), jnp.where(is_in, z + 2 * up, zz)
        return jnp.where(is_in, out_z, nxt), jnp.where(is_in, z, zz)

    tile = []
    for j in range(nz):
        zz = target(j)
        for h in range(nch):
            k = zz * nch + h
            mine = term(zz * 2 + y, h)
            y_copy(j, h).wait_recv()
            mine = mine + yr[j * nch + h].astype(F32)
            if j == nz - 1:
                z_copy(z, h, nxt, s1).wait_recv()
                z_copy(z, h, nxt, s2).wait_recv()
                mine = mine + zr[s1 * nch + h].astype(F32) + zr[s2 * nch + h].astype(F32)
                tile.append(mine.astype(BF))
                continue
            if j < 2:
                acc[k, :, :cw] = mine

                @pl.when(is_in)
                def _():
                    z_copy(zz, h, zz, zz).wait_recv()
                    acc[k, :, :cw] = acc[k, :, :cw] + zr[k].astype(F32)

                zs[k] = acc[k, :, :cw].astype(BF)
            else:
                zs[k] = mine.astype(BF)
            dz, slot = route(j)
            z_copy(zz, h, dz, slot).start()
    tile = jnp.concatenate(tile, axis=1)
    tile_out[...] = tile

    prod = mm(p_v[...].reshape(spn, width), tile, 1, 1)
    prod = jnp.sum(jnp.where(same_row((spn, tp)), prod, 0.0).reshape(nsrc, rows, tp), axis=1)
    fold = (
        outer(iota((ntask, tp), 1)) == iota((ntask, tp), 0)
    )
    part_w = mm(jnp.where(fold, 1.0, 0.0), prod, 1, 1, lax.Precision.HIGHEST)
    wp[...] = part_w
    wbuf[me] = part_w

    def w_copy(k):
        to = lax.rem(me + k, n)
        return remote(wp, wbuf.at[me], ws.at[k], wv.at[k], to // nmp, lax.rem(to, nmp))

    @pl.loop(1, n)
    def _(k):
        w_copy(k).start()

    w_save.wait()
    att_save.wait()

    for h in range(nch):
        g_copy(z, h, nxt).wait_send()
        f_copy(z, h, y).wait_send()
        t_copy(z, h).wait_send()

    @pl.loop(nch, steps)
    def _(i):
        zz, h = place(i)
        f_copy(zz, h, y).wait_send()

        @pl.when(is_in)
        def _():
            g_copy(zz, h, nxt).wait_send()

        @pl.when(is_in & (zz == out_z))
        def _():
            t_copy(zz, h).wait_send()

        u_copy(zz, h, nxt, s1).wait_send()

    @pl.when(is_in)
    def _():
        for h in range(nch):
            g2_copy(h).wait_send()

    for j in range(nz):
        for h in range(nch):
            y_copy(j, h).wait_send()
            if j < nz - 1:
                z_copy(target(j), h, nxt, s1).wait_send()

    @pl.loop(0, steps)
    def _(i):
        zz, h = place(i)

        @pl.loop(1, ne)
        def _(r):
            c_copy(zz, h, lax.rem(own + r, ne)).wait_send()

        @pl.when(is_in | (zz == z))
        def _():
            @pl.loop(1, ne)
            def _(r):
                b_copy(zz, h, lax.rem(own + r, ne), 0).wait_send()

        @pl.when(is_in & (zz != out_z))
        def _():
            @pl.loop(0, ne)
            def _(r):
                b_copy(zz, h, r, 1).wait_send()

    @pl.loop(1, n)
    def _(k):
        w_copy(k).wait()

    wg = jnp.sum(wbuf[...], axis=0)
    lg_out[...] = mix * (wg - jnp.sum(mix * wg, axis=1, keepdims=True))


def source_kernel(w_ref, tile_ref, att_ref, lg_ref, out_ref, att_out, lg_out):
    att_out[...] = att_ref[...]
    lg_out[...] = lg_ref[...]
    got = mm(w_ref[...], tile_ref[...], 0, 0)
    out_ref[...] = got.reshape(out_ref.shape)


def per_device(ndp, nmp, *args):
    source_prompts, task_logits, task_ids, key_weight, value_weight = args[:5]
    queries, keys, values, cotangent = args[5:]
    nsrc, ptok, width = source_prompts.shape
    ntask = task_logits.shape[0]
    ge = task_ids.shape[0]
    rows = ptok // ndp
    nch = 2
    if width % (nch * DH) or nmp != 8 or ndp & (ndp - 1) or ge != nmp or ptok % ndp or rows % 16 or rows & (rows - 1) or ntask * rows != 128:
        return on_device(*args)
    n, nz = ndp * nmp, nmp // 2
    ne, st, cw = n // nz, nz * nch, width // nch
    tp, spn = ntask * rows, nsrc * rows
    seq, full = queries.shape[1:]
    vmem = pl.BlockSpec(memory_space=pltpu.VMEM)
    hbm = pl.BlockSpec(memory_space=pl.ANY)
    dma = pltpu.SemaphoreType.DMA
    attended, tile, logits_grad, w_big = pl.pallas_call(
        functools.partial(chain_kernel, ndp, nmp, nch),
        out_shape=(
            jax.ShapeDtypeStruct((seq, full), BF),
            jax.ShapeDtypeStruct((tp, width), BF),
            jax.ShapeDtypeStruct((ntask, nsrc), F32),
            jax.ShapeDtypeStruct((tp, spn), BF),
        ),
        in_specs=[vmem, pl.BlockSpec(memory_space=pltpu.SMEM)] + [hbm] * 7,
        out_specs=(hbm, vmem, vmem, hbm),
        scratch_shapes=[
            pltpu.VMEM((seq, full), BF),
            pltpu.VMEM((tp, spn), BF),
            pltpu.VMEM((nsrc, rows, width), BF),
            pltpu.VMEM((full, width), BF),
            pltpu.VMEM((full, width), BF),
            pltpu.VMEM((seq, full), BF),
            pltpu.VMEM((seq, full), BF),
            pltpu.VMEM((seq, full), BF),
            pltpu.VMEM((seq, full), BF),
            pltpu.VMEM((nmp, nch, tp, cw), BF),
            pltpu.VMEM((ge, tp), F32),
            pltpu.VMEM((ndp, ge, tp), F32),
            pltpu.VMEM((st, tp, 2 * cw), BF),
            pltpu.VMEM((st, 2 * ne, 2, rows, cw), BF),
            pltpu.VMEM((2, ptok, full), BF),
            pltpu.VMEM((2, ptok, full), BF),
            pltpu.VMEM((st, ne, 2, rows, cw), BF),
            pltpu.VMEM((st, tp, 2 * cw), F32),
            pltpu.VMEM((st, tp, 2 * cw), BF),
            pltpu.VMEM((st, tp, 2 * cw), BF),
            pltpu.VMEM((st, tp, cw), BF),
            pltpu.VMEM((st, tp, cw), BF),
            pltpu.VMEM((st, tp, cw), BF),
            pltpu.VMEM((st, tp, cw), BF),
            pltpu.VMEM((ntask, nsrc), F32),
            pltpu.VMEM((n, ntask, nsrc), F32),
            dma((13,)),
            dma((st + nch,)), dma((st,)), dma((st,)), dma((st,)),
            dma((ndp,)), dma((ndp,)),
            dma((st,)), dma((st,)),
            dma((st * 2 * ne,)), dma((st * ne,)), dma((st * ne,)), dma((st * ne,)),
            dma((st,)), dma((st,)), dma((st,)), dma((st,)), dma((st,)), dma((st,)),
            dma((n,)), dma((n,)),
        ],
        compiler_params=pltpu.CompilerParams(
            collective_id=0, has_side_effects=True, vmem_limit_bytes=60 * 2**20
        ),
        name="chain",
    )(
        task_logits, task_ids, source_prompts, key_weight, value_weight,
        queries.reshape(seq, full), keys.reshape(seq, full),
        values.reshape(seq, full), cotangent.reshape(seq, full),
    )
    steps = 2
    source_grad, attended, logits_grad = pl.pallas_call(
        source_kernel,
        grid=(steps,),
        out_shape=(
            jax.ShapeDtypeStruct((nsrc, rows, width), F32),
            jax.ShapeDtypeStruct((seq, full), BF),
            jax.ShapeDtypeStruct((ntask, nsrc), F32),
        ),
        in_specs=[
            pl.BlockSpec((tp, spn // steps), lambda i: (0, i)),
            pl.BlockSpec((tp, width), lambda i: (0, 0)),
            pl.BlockSpec((seq // steps, full), lambda i: (i, 0)),
            pl.BlockSpec((ntask, nsrc), lambda i: (0, 0)),
        ],
        out_specs=(
            pl.BlockSpec((nsrc // steps, rows, width), lambda i: (i, 0, 0)),
            pl.BlockSpec((seq // steps, full), lambda i: (i, 0)),
            pl.BlockSpec((ntask, nsrc), lambda i: (0, 0)),
        ),
        name="source_grad",
    )(w_big, tile, attended, logits_grad)
    return (attended.reshape(queries.shape), source_grad, logits_grad)


def solution(mesh):
    placed = (
        P(None, None, "mp"),
        P(),
        P("dp"),
        P(None, "mp"),
        P(None, "mp"),
        P(("dp", "mp"), None, None),
        P(("dp", "mp"), None, None),
        P(("dp", "mp"), None, None),
        P(("dp", "mp"), None, None),
    )
    return jax.shard_map(
        functools.partial(per_device, mesh.shape["dp"], mesh.shape["mp"]),
        mesh=mesh,
        in_specs=placed,
        out_specs=(P(("dp", "mp"), None, None), P(None, "dp", "mp"), P()),
        check_vma=False,
    )
```

```python
import functools

import jax
import jax.numpy as jnp
from jax import lax
from jax.experimental import pallas as pl
from jax.experimental.pallas import tpu as pltpu
from jax.sharding import PartitionSpec as P

D = 4096
HEADS = 32
DH = 128
NSRC = 128
NTASK = 8
PTOK = 64
SEQ = 128
E_DEV = 1


mask_fill = -1e30


def example_block(prompt_pair, queries, keys, values, cotangent):
    examples = queries.shape[0]
    score_scale = DH ** (-0.5)
    key_all = jnp.concatenate([prompt_pair[:, :, 0, :], keys], axis=1)
    value_all = jnp.concatenate([prompt_pair[:, :, 1, :], values], axis=1)
    query_heads = queries.reshape(examples, SEQ, HEADS, DH)
    key_heads = key_all.reshape(examples, PTOK + SEQ, HEADS, DH)
    value_heads = value_all.reshape(examples, PTOK + SEQ, HEADS, DH)
    cot_heads = cotangent.reshape(examples, SEQ, HEADS, DH)
    scores = (
        jnp.einsum("eihd,ejhd->ehij", query_heads, key_heads, preferred_element_type=jnp.float32)
        * score_scale
    )
    column = jnp.arange(PTOK + SEQ)[None, :]
    position = jnp.arange(SEQ)[:, None]
    visible = (column < PTOK) | (column - PTOK <= position)
    scores = jnp.where(visible[None, None], scores, mask_fill)
    top_score = jnp.max(scores, axis=3, keepdims=True)
    exponent = jnp.exp(scores - top_score)
    attention = exponent / jnp.sum(exponent, axis=3, keepdims=True)
    attention_rounded = attention.astype(jnp.bfloat16)
    attended = jnp.einsum(
        "ehij,ejhd->eihd", attention_rounded, value_heads, preferred_element_type=jnp.float32
    )
    attended = attended.astype(jnp.bfloat16).reshape(examples, SEQ, D)
    grad_attention = jnp.einsum(
        "eihd,ejhd->ehij", cot_heads, value_heads, preferred_element_type=jnp.float32
    )
    inner_sum = jnp.sum(attention * grad_attention, axis=3, keepdims=True)
    grad_scores = (attention * (grad_attention - inner_sum)).astype(jnp.bfloat16)
    key_grads = jnp.einsum(
        "ehij,eihd->ejhd",
        grad_scores[:, :, :, :PTOK],
        query_heads,
        preferred_element_type=jnp.float32,
    )
    key_grads = (key_grads * score_scale).astype(jnp.bfloat16).reshape(examples, PTOK, D)
    value_grads = jnp.einsum(
        "ehij,eihd->ejhd",
        attention_rounded[:, :, :, :PTOK],
        cot_heads,
        preferred_element_type=jnp.float32,
    )
    value_grads = value_grads.astype(jnp.bfloat16).reshape(examples, PTOK, D)
    return (attended, jnp.stack([key_grads, value_grads], axis=2))


def tile_products(tile_grad, source_prompts, mix_weights, col_width):
    rows_here = tile_grad.shape[1]
    own_prompts = lax.dynamic_slice_in_dim(
        source_prompts, lax.axis_index("dp") * rows_here, rows_here, 1
    )
    tile_flat = tile_grad.reshape(NTASK, rows_here * col_width)
    source_grad = jnp.dot(mix_weights.T, tile_flat, precision=lax.Precision.HIGHEST)
    source_grad = source_grad.reshape(NSRC, rows_here, col_width)
    weight_part = jnp.dot(
        tile_flat,
        own_prompts.reshape(NSRC, rows_here * col_width).astype(jnp.float32).T,
        precision=lax.Precision.HIGHEST,
    )
    return (source_grad, weight_part)


def on_device(
    source_prompts,
    task_logits,
    task_ids,
    key_weight,
    value_weight,
    queries,
    keys,
    values,
    cotangent,
):
    col_width = key_weight.shape[1]
    group_examples = task_ids.shape[0]
    mix_weights = jax.nn.softmax(task_logits, axis=1)
    mix_rounded = mix_weights.astype(jnp.bfloat16)
    mixture = jnp.dot(
        mix_rounded,
        source_prompts.reshape(NSRC, PTOK * col_width),
        preferred_element_type=jnp.float32,
    )
    mixture = mixture.astype(jnp.bfloat16).reshape(NTASK, PTOK, col_width)
    pair_weight = jnp.concatenate([key_weight, value_weight], axis=1)
    portion = lax.all_gather(mixture, "mp", axis=2, tiled=True)
    portion_rows = portion.reshape(NTASK * PTOK, portion.shape[2])
    projected = jnp.dot(portion_rows, pair_weight, preferred_element_type=jnp.float32)
    projected = projected.astype(jnp.bfloat16).reshape(NTASK, PTOK, 2, col_width)
    task_range = jnp.arange(NTASK, dtype=jnp.int32)
    selector_all = (task_ids[:, None] == task_range[None, :]).astype(jnp.bfloat16)
    table_full = lax.all_gather(projected, "mp", axis=3, tiled=True)
    own_offset = lax.axis_index("mp") * E_DEV
    own_selector = lax.dynamic_slice_in_dim(selector_all, own_offset, E_DEV, 0)
    chosen = jnp.dot(
        own_selector, table_full.reshape(NTASK, PTOK * 2 * D), preferred_element_type=jnp.float32
    )
    prompt_pair = chosen.astype(jnp.bfloat16).reshape(E_DEV, PTOK, 2, D)
    attended, outgoing_grads = example_block(prompt_pair, queries, keys, values, cotangent)
    incoming = lax.all_to_all(outgoing_grads, "mp", split_axis=3, concat_axis=0, tiled=True)
    group_grads = jnp.dot(
        selector_all.T,
        incoming.reshape(group_examples, PTOK * 2 * col_width),
        preferred_element_type=jnp.float32,
    )
    pair_weight_t = pair_weight.astype(jnp.float32).T
    task_rows = lax.psum_scatter(
        group_grads.reshape(NTASK, PTOK, 2 * col_width), "dp", scatter_dimension=1, tiled=True
    )
    rows_here = task_rows.shape[1]
    row_terms = jnp.dot(
        task_rows.reshape(NTASK * rows_here, 2 * col_width),
        pair_weight_t,
        precision=lax.Precision.HIGHEST,
    ).reshape(NTASK, rows_here, D)
    tile_grad = lax.psum_scatter(row_terms, "mp", scatter_dimension=2, tiled=True)
    source_grad, weight_part = tile_products(tile_grad, source_prompts, mix_weights, col_width)
    weight_grad = lax.psum(weight_part, ("dp", "mp"))
    logits_grad = mix_weights * (
        weight_grad - jnp.sum(mix_weights * weight_grad, axis=1, keepdims=True)
    )
    return (attended, source_grad, logits_grad)


BF = jnp.bfloat16
F32 = jnp.float32


def mm(a, b, ca=1, cb=0, precision=None):
    return lax.dot_general(
        a, b, (((ca,), (cb,)), ((), ())), preferred_element_type=F32, precision=precision
    )


def chain_kernel(
    ndp, nmp, nch,
    lg_hbm, ids_hbm, sp_hbm, kw_hbm, vw_hbm, q_hbm, k_hbm, v_hbm, c_hbm,
    att_hbm, tile_hbm, lg_out, w_hbm,
    logits, ids_in, tile_v, att_out, w_out, p_v, kw_v, vw_v, q_v, k_v, v_v, c_v,
    mixed, ids_own, ids_buf, tab, sbuf, pair, gr, rbuf, acc, ubuf, urec, ys, yr, zs, zr, zt, wp, wbuf,
    lsem, gs, gv, fs, fv, js, jv, ts, tv, bs, bv, cs, cv, us, uv, hs, hv, es, ev, ws, wv,
):
    n = ndp * nmp
    nz = nmp // 2
    ne = n // nz
    width = kw_v.shape[1]
    cw = width // nch
    rows = p_v.shape[1]
    nsrc = p_v.shape[0]
    ntask = logits.shape[0]
    tp = ntask * rows
    spn = nsrc * rows
    seq = q_v.shape[0]
    steps = nz * nch
    d = lax.axis_index("dp")
    m = lax.axis_index("mp")
    z = m // 2
    y = lax.rem(m, 2)
    me = d * nmp + m
    own = y * ndp + d
    up = 1 - 2 * (z // 2)
    inner = lax.rem((z + 1) // 2, 2)
    is_in = inner == 1
    nxt = z + up
    out_z = z - up * inner
    other = z * 2 + (1 - y)

    shift = rows.bit_length() - 1

    def iota(shape, axis):
        return lax.broadcasted_iota(jnp.int32, shape, axis)

    def outer(a):
        return lax.shift_right_logical(a, jnp.int32(shift))

    def same_row(shape):
        return ((iota(shape, 0) ^ iota(shape, 1)) & (rows - 1)) == 0

    def remote(src, dst, ss, rs, dd, mm_):
        return pltpu.make_async_remote_copy(
            src_ref=src, dst_ref=dst, send_sem=ss, recv_sem=rs,
            device_id=(dd, mm_), device_id_type=pl.DeviceIdType.MESH,
        )

    def drain(ref, sem):
        pltpu.make_async_copy(ref, ref, sem).wait()

    def place(i):
        i = jnp.int32(i)
        k = i // nch
        off_in = jnp.where(k == 2, -1, jnp.where(k == 3, 2, k))
        return z + up * (inner * off_in + (1 - inner) * k), lax.rem(i, nch)

    small = [
        pltpu.make_async_copy(lg_hbm, logits, lsem.at[9]),
        pltpu.make_async_copy(ids_hbm, ids_in, lsem.at[10]),
    ]
    for c in small:
        c.start()
    npl = 4
    loads = []
    for i in range(npl):
        s_at = pl.ds(i * (nsrc // npl), nsrc // npl)
        loads.append(
            pltpu.make_async_copy(
                sp_hbm.at[s_at, pl.ds(pl.multiple_of(d * rows, rows), rows), :],
                p_v.at[s_at], lsem.at[0],
            )
        )
        loads[i].start()
    for i, (a, b) in enumerate(
        ((kw_hbm, kw_v), (vw_hbm, vw_v), (k_hbm, k_v), (q_hbm, q_v), (v_hbm, v_v), (c_hbm, c_v))
    ):
        loads.append(pltpu.make_async_copy(a, b, lsem.at[1 + i]))

    def turn(i):
        i = jnp.int32(i)
        zz, h = place(i)
        late = z + up * lax.rem(i // nch + 1, nz)
        return jnp.where(is_in, zz, late), h

    barrier = pltpu.get_barrier_semaphore()

    @pl.loop(1, n)
    def _(k):
        to = lax.rem(me + k, n)
        pl.semaphore_signal(
            barrier, inc=1, device_id=(to // nmp, lax.rem(to, nmp)),
            device_id_type=pl.DeviceIdType.MESH,
        )

    for c in small:
        c.wait()
    lg = logits[...]
    ex = jnp.exp(lg - jnp.max(lg, axis=1, keepdims=True))
    mix = ex / jnp.sum(ex, axis=1, keepdims=True)
    upm = (
        outer(iota((tp, ntask), 0)) == iota((tp, ntask), 1)
    )
    tall = mm(jnp.where(upm, 1.0, 0.0), mix.astype(BF).astype(F32)).astype(BF)
    out = (
        outer(iota((nsrc, spn), 1)) == iota((nsrc, spn), 0)
    )
    wide = mm(tall, jnp.where(out, 1.0, 0.0).astype(BF))
    w_out[...] = jnp.where(same_row((tp, spn)), wide, 0.0).astype(BF)
    for j in range(ids_in.shape[0]):
        line = jnp.full((1, tp), ids_in[j], jnp.int32).astype(F32)
        ids_own[pl.ds(j, 1), :] = line
        ids_buf[d, pl.ds(j, 1), :] = line

    pltpu.make_async_copy(p_v, p_v, lsem.at[0]).wait()
    for c in loads[npl:]:
        c.start()
    w_save = pltpu.make_async_copy(w_out, w_hbm, lsem.at[7])
    w_save.start()
    for h in range(nch):
        mixed[m, h] = mm(w_out[...], p_v[:, :, pl.ds(h * cw, cw)].reshape(spn, cw)).astype(BF)

    pl.semaphore_wait(barrier, n - 1)

    def g_copy(zz, h, dz):
        slot = zz * 2 + y
        return remote(
            mixed.at[slot, h], mixed.at[slot, h], gs.at[0], gv.at[zz * nch + h], d, dz * 2 + y
        )

    def f_copy(zz, h, yy):
        slot = zz * 2 + yy
        return remote(
            mixed.at[slot, h], mixed.at[slot, h], fs.at[0], fv.at[zz * nch + h], d, other
        )

    for h in range(nch):
        f_copy(z, h, y).start()

        @pl.when(is_in)
        def _():
            g_copy(z, h, out_z).start()
            g_copy(z, h, nxt).start()

        @pl.when(jnp.logical_not(is_in))
        def _():
            g_copy(z, h, nxt).start()

    @pl.when(jnp.logical_not(is_in))
    def _():
        for h in range(nch):
            g_copy(z, h, z + 3 * up).start()

    for j in range(1, ndp):
        remote(ids_own, ids_buf.at[d], js.at[0], jv.at[0], lax.rem(d + j, ndp), m).start()
    loads[npl].wait()
    loads[npl + 1].wait()

    def part(slot, h):
        block = mixed[slot, h]
        at = pl.ds(pl.multiple_of(slot * width + h * cw, cw), cw)
        return mm(block, kw_v[at, :]), mm(block, vw_v[at, :])

    pk, pv = part(m, 0)
    for h in range(1, nch):
        a, b = part(m, h)
        pk, pv = pk + a, pv + b
    arrive = [(0, 0, h, h) for h in range(nch)]
    arrive += [(1, 1 - 2 * (i % 2), i, i // 2) for i in range(nch)]
    for i in range(2 * nch):
        k = nch + i
        side = (1 - 2 * (k % 2), k // 2) if k < 2 * nch else (2, k - 2 * nch)
        arrive.append((2 + i % 2, side[0], i // 2, side[1]))

    def arrival(i):
        off_o, off_i, h_o, h_i = arrive[i]
        return z + up * (off_o + inner * (off_i - off_o)), h_o + inner * (h_i - h_o)

    def from_z(i, pk, pv):
        zz, h = arrival(i)
        g_copy(zz, h, nxt).wait_recv()
        if arrive[i][1] != 2:
            @pl.when(is_in)
            def _():
                g_copy(zz, h, out_z if arrive[i][1] == 1 else nxt).start()

        f_copy(zz, h, y).start()
        a, b = part(zz * 2 + y, h)
        return pk + a, pv + b

    def from_y(i, pk, pv):
        zz, h = arrival(i)
        f_copy(zz, h, 1 - y).wait_recv()
        a, b = part(zz * 2 + (1 - y), h)
        return pk + a, pv + b

    lag = 2 * nch
    for i in range(nch, steps + lag):
        if i < steps:
            pk, pv = from_z(i, pk, pv)
        if i >= lag:
            pk, pv = from_y(i - lag, pk, pv)
    for h in range(nch):
        at = slice(h * cw, (h + 1) * cw)
        tab[z * nch + h, :, :cw] = pk[:, at].astype(BF)
        tab[z * nch + h, :, cw:] = pv[:, at].astype(BF)
        remote(
            tab.at[z * nch + h], tab.at[z * nch + h], ts.at[0], tv.at[z * nch + h],
            d, nxt * 2 + y,
        ).start()
    drain(ids_buf.at[pl.ds(0, ndp - 1)], jv.at[0])

    ids_all = ids_buf[...].reshape(n, tp).astype(BF)
    q_rows = 2 * ne * rows
    q = outer(iota((q_rows, n), 0))
    q_z = jnp.where(q < ne, z, out_z)
    q_in = q & (ne - 1)
    q_dev = lax.rem(q_in, jnp.int32(ndp)) * nmp + q_z * 2 + q_in // jnp.int32(ndp)
    ids_x = mm(jnp.where(q_dev == iota((q_rows, n), 1), 1.0, 0.0).astype(BF), ids_all)
    sel = jnp.where(
        (ids_x == outer(iota((q_rows, tp), 1)).astype(F32)) & same_row((q_rows, tp)), 1.0, 0.0
    ).astype(BF)
    sel_own = sel[: ne * rows]

    def row_at(dd):
        return pl.ds(pl.multiple_of(dd * rows, rows), rows)

    def col_at(zz, yy, h):
        return pl.ds(pl.multiple_of((zz * 2 + yy) * width + h * cw, cw), cw)

    def t_copy(zz, h, dz):
        k = zz * nch + h
        return remote(tab.at[k], tab.at[k], ts.at[0], tv.at[k], d, dz * 2 + y)

    def b_copy(zz, h, e, to_out):
        k = zz * nch + h
        g = e + to_out * ne
        return remote(
            sbuf.at[k * 2 * ne + g], pair.at[:, row_at(d), col_at(zz, y, h)],
            bs.at[0], bv.at[k],
            lax.rem(e, ndp), (out_z if to_out else z) * 2 + e // ndp,
        )

    def relay(i):
        zz, h = place(i)
        k = zz * nch + h

        @pl.when(zz != z)
        def _():
            t_copy(zz, h, nxt).wait_recv()

        @pl.when(is_in & (zz == out_z))
        def _():
            t_copy(zz, h, nxt).start()

        got = mm(sel, tab[k]).astype(BF)
        to = pl.ds(k * 2 * ne, 2 * ne)
        sbuf[to, 0] = got[:, :cw].reshape(2 * ne, rows, cw)
        sbuf[to, 1] = got[:, cw:].reshape(2 * ne, rows, cw)

        @pl.loop(1, ne)
        def _(r):
            b_copy(zz, h, lax.rem(own + r, ne), 0).start()

        pair[:, row_at(d), col_at(zz, y, h)] = sbuf[k * 2 * ne + own]

    def outward(i, first, count):
        zz, h = place(i)

        @pl.when(zz != out_z)
        def _():
            @pl.loop(first, first + count)
            def _(r):
                b_copy(zz, h, lax.rem(y * ndp + r, ne), 1).start()

    for i in range(nch):
        relay(i)

    @pl.when(is_in)
    def _():
        for side in range(2):
            for i in range(nch):
                outward(i, side * ndp, ndp)

    for c in loads[npl + 2:]:
        c.wait()

    def c_copy(zz, h, e):
        k = zz * nch + h
        return remote(
            gr.at[:, row_at(lax.rem(e, ndp)), col_at(zz, e // ndp, h)], rbuf.at[k * ne + own],
            cs.at[0], cv.at[k], lax.rem(e, ndp), z * 2 + e // ndp,
        )

    scale = DH ** (-0.5)
    to_exp2 = scale * 1.4426950408889634
    ptok = pair.shape[1]
    seen = iota((seq, seq), 0) <= iota((seq, seq), 1)

    def group(i):
        zz, h = turn(i)

        @pl.when(is_in | (zz == z))
        def _():
            drain(rbuf.at[pl.ds(0, ne - 1)], bv.at[zz * nch + h])

        @pl.when(jnp.logical_not(is_in | (zz == z)))
        def _():
            drain(rbuf.at[pl.ds(0, ne)], bv.at[zz * nch + h])

        ats, st, gt, va = [], [], [], []
        for yy in range(2):
            for hh in range(cw // DH):
                base = (zz * 2 + yy) * width + h * cw + hh * DH
                at = pl.ds(pl.multiple_of(base, DH), DH)
                ats.append(at)
                ka = jnp.concatenate([pair[0, :, at], k_v[:, at]], axis=0)
                va.append(jnp.concatenate([pair[1, :, at], v_v[:, at]], axis=0))
                st.append(mm(ka, q_v[:, at], 1, 1))
                gt.append(mm(va[-1], c_v[:, at], 1, 1))
        for j, at in enumerate(ats):
            s = st[j] * to_exp2
            s = jnp.concatenate([s[:ptok], jnp.where(seen, s[ptok:], mask_fill)], axis=0)
            e = jnp.exp2(s - jnp.max(s, axis=0, keepdims=True))
            a = e * (1.0 / jnp.sum(e, axis=0, keepdims=True))
            ab = a.astype(BF)
            inner_sum = jnp.sum(a * gt[j], axis=0, keepdims=True)
            gs1 = (a[:ptok] * (gt[j][:ptok] - inner_sum)).astype(BF)
            gr[0, :, at] = (mm(gs1, q_v[:, at]) * scale).astype(BF)
            gr[1, :, at] = mm(ab[:ptok], c_v[:, at]).astype(BF)
            att_out[:, at] = mm(ab, va[j], 0, 0).astype(BF)

        @pl.loop(1, ne)
        def _(r):
            c_copy(zz, h, lax.rem(own + r, ne)).start()

        rbuf[(zz * nch + h) * ne + own] = gr[:, row_at(d), col_at(zz, y, h)]

    def u_copy(zz, h, dz, slot):
        k = zz * nch + h
        return remote(
            ubuf.at[k], urec.at[slot * nch + h], us.at[0], uv.at[slot * nch + h], d, dz * 2 + y
        )

    def total(i):
        zz, h = turn(i)
        k = zz * nch + h

        drain(rbuf.at[pl.ds(0, ne - 1)], cv.at[k])
        at = pl.ds(k * ne, ne)
        acc[k, :, :cw] = mm(sel_own, rbuf[at, 0].reshape(ne * rows, cw), 0, 0)
        acc[k, :, cw:] = mm(sel_own, rbuf[at, 1].reshape(ne * rows, cw), 0, 0)

        @pl.when(is_in & (zz == out_z))
        def _():
            ubuf[k] = acc[k].astype(BF)
            u_copy(zz, h, zz, z).start()

        @pl.when(jnp.logical_not(is_in | (zz == z)))
        def _():
            ubuf[k] = acc[k].astype(BF)
            u_copy(zz, h, nxt, zz).start()

    def combine(i):
        zz, h = turn(i)
        k = zz * nch + h
        u_copy(zz, h, nxt, zz).wait_recv()
        ubuf[k] = (acc[k] + urec[k].astype(F32)).astype(BF)
        u_copy(zz, h, zz, jnp.where(zz == nxt, z + 2 * up, z)).start()

    ahead = 2 * nch

    @pl.when(is_in)
    def _():
        @pl.loop(nch, ahead)
        def _(i):
            relay(i)
            outward(i, 0, ne)

    @pl.loop(0, steps)
    def _(i):
        group(i)

        @pl.when(is_in & (i < steps - ahead))
        def _():
            relay(i + ahead)
            outward(i + ahead, 0, ne)

        @pl.when(i >= nch)
        def _():
            total(i - nch)

        @pl.when(is_in & (i >= 3 * nch))
        def _():
            combine(i - 2 * nch)

    att_save = pltpu.make_async_copy(att_out, att_hbm, lsem.at[8])
    att_save.start()

    @pl.loop(steps - nch, steps)
    def _(i):
        total(i)

    @pl.when(is_in)
    def _():
        @pl.loop(steps - nch, steps)
        def _(i):
            combine(i)

    s1 = z + up * (1 - inner)
    s2 = z + up * (2 - 3 * inner)
    tks, tvs = [], []
    for h in range(nch):
        u_copy(z, h, nxt, s1).wait_recv()
        u_copy(z, h, nxt, s2).wait_recv()
        k = z * nch + h
        acc[k] = acc[k] + urec[s1 * nch + h].astype(F32) + urec[s2 * nch + h].astype(F32)

        t = acc[k].astype(BF)
        tks.append(t[:, :cw])
        tvs.append(t[:, cw:])
    tk = jnp.concatenate(tks, axis=1)
    tv_ = jnp.concatenate(tvs, axis=1)

    def term(slot):
        at = pl.ds(pl.multiple_of(slot * width, width), width)
        return mm(tk, kw_v[at, :], 1, 1) + mm(tv_, vw_v[at, :], 1, 1)

    def target(j):
        return z + up * ((nz - 1 - j) * (1 - inner) + inner * (2, 1, -1, 0)[j])

    def y_copy(j, h):
        k = j * nch + h
        return remote(ys.at[k], yr.at[k], hs.at[0], hv.at[k], d, other)

    def z_copy(zz, h, dz, slot):
        k = zz * nch + h
        return remote(
            zs.at[k], zr.at[slot * nch + h], es.at[0], ev.at[slot * nch + h], d, dz * 2 + y
        )

    for j in range(nz):
        got = term(target(j) * 2 + (1 - y)).astype(BF)
        for h in range(nch):
            ys[j * nch + h] = got[:, h * cw : (h + 1) * cw]
            y_copy(j, h).start()
    for j in range(nz):
        zt[j] = term(target(j) * 2 + y)

    def route(j):
        zz = target(j)
        if j == 0:
            return jnp.where(is_in, zz, nxt), jnp.where(is_in, z, zz)
        if j == 1:
            return jnp.where(is_in, zz, nxt), jnp.where(is_in, z + 2 * up, zz)
        return jnp.where(is_in, out_z, nxt), jnp.where(is_in, z, zz)

    tile = []
    for j in range(nz):
        zz = target(j)
        for h in range(nch):
            k = zz * nch + h
            y_copy(j, h).wait_recv()
            mine = zt[j, :, h * cw : (h + 1) * cw] + yr[j * nch + h].astype(F32)
            if j == nz - 1:
                z_copy(z, h, nxt, s1).wait_recv()
                z_copy(z, h, nxt, s2).wait_recv()
                mine = mine + zr[s1 * nch + h].astype(F32) + zr[s2 * nch + h].astype(F32)
                tile.append(mine.astype(BF))
                continue
            if j < 2:
                acc[k, :, :cw] = mine

                @pl.when(is_in)
                def _():
                    z_copy(zz, h, zz, zz).wait_recv()
                    acc[k, :, :cw] = acc[k, :, :cw] + zr[k].astype(F32)

                zs[k] = acc[k, :, :cw].astype(BF)
            else:
                zs[k] = mine.astype(BF)
            dz, slot = route(j)
            z_copy(zz, h, dz, slot).start()
    tile = jnp.concatenate(tile, axis=1)
    tile_v[...] = tile
    tile_save = pltpu.make_async_copy(tile_v, tile_hbm, lsem.at[11])
    tile_save.start()

    prod = mm(p_v[...].reshape(spn, width), tile, 1, 1)
    prod = jnp.sum(jnp.where(same_row((spn, tp)), prod, 0.0).reshape(nsrc, rows, tp), axis=1)
    fold = (
        outer(iota((ntask, tp), 1)) == iota((ntask, tp), 0)
    )
    part_w = mm(jnp.where(fold, 1.0, 0.0), prod, 1, 1, lax.Precision.HIGHEST)
    wp[...] = part_w
    wbuf[me] = part_w

    def w_copy(k):
        to = lax.rem(me + k, n)
        return remote(wp, wbuf.at[me], ws.at[0], wv.at[0], to // nmp, lax.rem(to, nmp))

    @pl.loop(1, n)
    def _(k):
        w_copy(k).start()

    w_save.wait()
    att_save.wait()
    tile_save.wait()

    moved = steps - nch
    drain(mixed.at[pl.ds(0, nz)], fs.at[0])
    drain(ids_buf.at[pl.ds(0, ndp - 1)], js.at[0])
    drain(rbuf.at[pl.ds(0, steps * (ne - 1))], cs.at[0])
    drain(ubuf.at[pl.ds(0, moved)], us.at[0])
    drain(ys, hs.at[0])
    drain(zs.at[pl.ds(0, moved)], es.at[0])

    @pl.when(is_in)
    def _():
        drain(mixed.at[pl.ds(0, nz)], gs.at[0])
        drain(tab.at[pl.ds(0, 2 * nch)], ts.at[0])
        drain(sbuf.at[pl.ds(0, steps * (ne - 1) + moved * ne)], bs.at[0])

    @pl.when(jnp.logical_not(is_in))
    def _():
        drain(mixed.at[pl.ds(0, nz // 2)], gs.at[0])
        drain(tab.at[pl.ds(0, nch)], ts.at[0])
        drain(sbuf.at[pl.ds(0, nch * (ne - 1))], bs.at[0])

    drain(wbuf.at[pl.ds(0, n - 1)], ws.at[0])
    drain(wbuf.at[pl.ds(0, n - 1)], wv.at[0])

    wg = jnp.sum(wbuf[...], axis=0)
    lg_out[...] = mix * (wg - jnp.sum(mix * wg, axis=1, keepdims=True))


def source_kernel(w_ref, tile_ref, att_ref, lg_ref, out_ref, att_out, lg_out):
    att_out[...] = att_ref[...]
    lg_out[...] = lg_ref[...]
    got = mm(w_ref[...], tile_ref[...], 0, 0)
    out_ref[...] = got.reshape(out_ref.shape)


def per_device(ndp, nmp, *args):
    source_prompts, task_logits, task_ids, key_weight, value_weight = args[:5]
    queries, keys, values, cotangent = args[5:]
    nsrc, ptok, width = source_prompts.shape
    ntask = task_logits.shape[0]
    ge = task_ids.shape[0]
    rows = ptok // ndp
    nch = 2
    if width % (nch * DH) or nmp != 8 or ndp & (ndp - 1) or ge != nmp or ptok % ndp or rows % 16 or rows & (rows - 1) or ntask * rows != 128:
        return on_device(*args)
    n, nz = ndp * nmp, nmp // 2
    ne, st, cw = n // nz, nz * nch, width // nch
    tp, spn = ntask * rows, nsrc * rows
    seq, full = queries.shape[1:]
    vmem = pl.BlockSpec(memory_space=pltpu.VMEM)
    hbm = pl.BlockSpec(memory_space=pl.ANY)
    dma = pltpu.SemaphoreType.DMA
    attended, tile, logits_grad, w_big = pl.pallas_call(
        functools.partial(chain_kernel, ndp, nmp, nch),
        out_shape=(
            jax.ShapeDtypeStruct((seq, full), BF),
            jax.ShapeDtypeStruct((tp, width), BF),
            jax.ShapeDtypeStruct((ntask, nsrc), F32),
            jax.ShapeDtypeStruct((tp, spn), BF),
        ),
        in_specs=[hbm] * 9,
        out_specs=(hbm, hbm, vmem, hbm),
        scratch_shapes=[
            pltpu.VMEM((ntask, nsrc), F32),
            pltpu.SMEM((ge,), jnp.int32),
            pltpu.VMEM((tp, width), BF),
            pltpu.VMEM((seq, full), BF),
            pltpu.VMEM((tp, spn), BF),
            pltpu.VMEM((nsrc, rows, width), BF),
            pltpu.VMEM((full, width), BF),
            pltpu.VMEM((full, width), BF),
            pltpu.VMEM((seq, full), BF),
            pltpu.VMEM((seq, full), BF),
            pltpu.VMEM((seq, full), BF),
            pltpu.VMEM((seq, full), BF),
            pltpu.VMEM((nmp, nch, tp, cw), BF),
            pltpu.VMEM((ge, tp), F32),
            pltpu.VMEM((ndp, ge, tp), F32),
            pltpu.VMEM((st, tp, 2 * cw), BF),
            pltpu.VMEM((st * 2 * ne, 2, rows, cw), BF),
            pltpu.VMEM((2, ptok, full), BF),
            pltpu.VMEM((2, ptok, full), BF),
            pltpu.VMEM((st * ne, 2, rows, cw), BF),
            pltpu.VMEM((st, tp, 2 * cw), F32),
            pltpu.VMEM((st, tp, 2 * cw), BF),
            pltpu.VMEM((st, tp, 2 * cw), BF),
            pltpu.VMEM((st, tp, cw), BF),
            pltpu.VMEM((st, tp, cw), BF),
            pltpu.VMEM((st, tp, cw), BF),
            pltpu.VMEM((st, tp, cw), BF),
            pltpu.VMEM((nz, tp, width), F32),
            pltpu.VMEM((ntask, nsrc), F32),
            pltpu.VMEM((n, ntask, nsrc), F32),
            dma((12,)),
            dma((1,)), dma((st,)), dma((1,)), dma((st,)), dma((1,)), dma((1,)),
            dma((1,)), dma((st,)), dma((1,)), dma((st,)), dma((1,)), dma((st,)),
            dma((1,)), dma((st,)), dma((1,)), dma((st,)), dma((1,)), dma((st,)),
            dma((1,)), dma((1,)),
        ],
        compiler_params=pltpu.CompilerParams(
            collective_id=0, has_side_effects=True, vmem_limit_bytes=60 * 2**20
        ),
        name="chain",
    )(
        task_logits, task_ids, source_prompts, key_weight, value_weight,
        queries.reshape(seq, full), keys.reshape(seq, full),
        values.reshape(seq, full), cotangent.reshape(seq, full),
    )
    steps = 2
    source_grad, attended, logits_grad = pl.pallas_call(
        source_kernel,
        grid=(steps,),
        out_shape=(
            jax.ShapeDtypeStruct((nsrc, rows, width), F32),
            jax.ShapeDtypeStruct((seq, full), BF),
            jax.ShapeDtypeStruct((ntask, nsrc), F32),
        ),
        in_specs=[
            pl.BlockSpec((tp, spn // steps), lambda i: (0, i)),
            pl.BlockSpec((tp, width), lambda i: (0, 0)),
            pl.BlockSpec((seq // steps, full), lambda i: (i, 0)),
            pl.BlockSpec((ntask, nsrc), lambda i: (0, 0)),
        ],
        out_specs=(
            pl.BlockSpec((nsrc // steps, rows, width), lambda i: (i, 0, 0)),
            pl.BlockSpec((seq // steps, full), lambda i: (i, 0)),
            pl.BlockSpec((ntask, nsrc), lambda i: (0, 0)),
        ),
        name="source_grad",
    )(w_big, tile, attended, logits_grad)
    return (attended.reshape(queries.shape), source_grad, logits_grad)


def solution(mesh):
    placed = (
        P(None, None, "mp"),
        P(),
        P("dp"),
        P(None, "mp"),
        P(None, "mp"),
        P(("dp", "mp"), None, None),
        P(("dp", "mp"), None, None),
        P(("dp", "mp"), None, None),
        P(("dp", "mp"), None, None),
    )
    return jax.shard_map(
        functools.partial(per_device, mesh.shape["dp"], mesh.shape["mp"]),
        mesh=mesh,
        in_specs=placed,
        out_specs=(P(("dp", "mp"), None, None), P(None, "dp", "mp"), P()),
        check_vma=False,
    )
```

```python
import functools

import jax
import jax.numpy as jnp
from jax import lax
from jax.experimental import pallas as pl
from jax.experimental.pallas import tpu as pltpu
from jax.sharding import PartitionSpec as P

D = 4096
HEADS = 32
DH = 128
NSRC = 128
NTASK = 8
PTOK = 64
SEQ = 128
E_DEV = 1


mask_fill = -1e30


def example_block(prompt_pair, queries, keys, values, cotangent):
    examples = queries.shape[0]
    score_scale = DH ** (-0.5)
    key_all = jnp.concatenate([prompt_pair[:, :, 0, :], keys], axis=1)
    value_all = jnp.concatenate([prompt_pair[:, :, 1, :], values], axis=1)
    query_heads = queries.reshape(examples, SEQ, HEADS, DH)
    key_heads = key_all.reshape(examples, PTOK + SEQ, HEADS, DH)
    value_heads = value_all.reshape(examples, PTOK + SEQ, HEADS, DH)
    cot_heads = cotangent.reshape(examples, SEQ, HEADS, DH)
    scores = (
        jnp.einsum("eihd,ejhd->ehij", query_heads, key_heads, preferred_element_type=jnp.float32)
        * score_scale
    )
    column = jnp.arange(PTOK + SEQ)[None, :]
    position = jnp.arange(SEQ)[:, None]
    visible = (column < PTOK) | (column - PTOK <= position)
    scores = jnp.where(visible[None, None], scores, mask_fill)
    top_score = jnp.max(scores, axis=3, keepdims=True)
    exponent = jnp.exp(scores - top_score)
    attention = exponent / jnp.sum(exponent, axis=3, keepdims=True)
    attention_rounded = attention.astype(jnp.bfloat16)
    attended = jnp.einsum(
        "ehij,ejhd->eihd", attention_rounded, value_heads, preferred_element_type=jnp.float32
    )
    attended = attended.astype(jnp.bfloat16).reshape(examples, SEQ, D)
    grad_attention = jnp.einsum(
        "eihd,ejhd->ehij", cot_heads, value_heads, preferred_element_type=jnp.float32
    )
    inner_sum = jnp.sum(attention * grad_attention, axis=3, keepdims=True)
    grad_scores = (attention * (grad_attention - inner_sum)).astype(jnp.bfloat16)
    key_grads = jnp.einsum(
        "ehij,eihd->ejhd",
        grad_scores[:, :, :, :PTOK],
        query_heads,
        preferred_element_type=jnp.float32,
    )
    key_grads = (key_grads * score_scale).astype(jnp.bfloat16).reshape(examples, PTOK, D)
    value_grads = jnp.einsum(
        "ehij,eihd->ejhd",
        attention_rounded[:, :, :, :PTOK],
        cot_heads,
        preferred_element_type=jnp.float32,
    )
    value_grads = value_grads.astype(jnp.bfloat16).reshape(examples, PTOK, D)
    return (attended, jnp.stack([key_grads, value_grads], axis=2))


def tile_products(tile_grad, source_prompts, mix_weights, col_width):
    rows_here = tile_grad.shape[1]
    own_prompts = lax.dynamic_slice_in_dim(
        source_prompts, lax.axis_index("dp") * rows_here, rows_here, 1
    )
    tile_flat = tile_grad.reshape(NTASK, rows_here * col_width)
    source_grad = jnp.dot(mix_weights.T, tile_flat, precision=lax.Precision.HIGHEST)
    source_grad = source_grad.reshape(NSRC, rows_here, col_width)
    weight_part = jnp.dot(
        tile_flat,
        own_prompts.reshape(NSRC, rows_here * col_width).astype(jnp.float32).T,
        precision=lax.Precision.HIGHEST,
    )
    return (source_grad, weight_part)


def on_device(
    source_prompts,
    task_logits,
    task_ids,
    key_weight,
    value_weight,
    queries,
    keys,
    values,
    cotangent,
):
    col_width = key_weight.shape[1]
    group_examples = task_ids.shape[0]
    mix_weights = jax.nn.softmax(task_logits, axis=1)
    mix_rounded = mix_weights.astype(jnp.bfloat16)
    mixture = jnp.dot(
        mix_rounded,
        source_prompts.reshape(NSRC, PTOK * col_width),
        preferred_element_type=jnp.float32,
    )
    mixture = mixture.astype(jnp.bfloat16).reshape(NTASK, PTOK, col_width)
    pair_weight = jnp.concatenate([key_weight, value_weight], axis=1)
    portion = lax.all_gather(mixture, "mp", axis=2, tiled=True)
    portion_rows = portion.reshape(NTASK * PTOK, portion.shape[2])
    projected = jnp.dot(portion_rows, pair_weight, preferred_element_type=jnp.float32)
    projected = projected.astype(jnp.bfloat16).reshape(NTASK, PTOK, 2, col_width)
    task_range = jnp.arange(NTASK, dtype=jnp.int32)
    selector_all = (task_ids[:, None] == task_range[None, :]).astype(jnp.bfloat16)
    table_full = lax.all_gather(projected, "mp", axis=3, tiled=True)
    own_offset = lax.axis_index("mp") * E_DEV
    own_selector = lax.dynamic_slice_in_dim(selector_all, own_offset, E_DEV, 0)
    chosen = jnp.dot(
        own_selector, table_full.reshape(NTASK, PTOK * 2 * D), preferred_element_type=jnp.float32
    )
    prompt_pair = chosen.astype(jnp.bfloat16).reshape(E_DEV, PTOK, 2, D)
    attended, outgoing_grads = example_block(prompt_pair, queries, keys, values, cotangent)
    incoming = lax.all_to_all(outgoing_grads, "mp", split_axis=3, concat_axis=0, tiled=True)
    group_grads = jnp.dot(
        selector_all.T,
        incoming.reshape(group_examples, PTOK * 2 * col_width),
        preferred_element_type=jnp.float32,
    )
    pair_weight_t = pair_weight.astype(jnp.float32).T
    task_rows = lax.psum_scatter(
        group_grads.reshape(NTASK, PTOK, 2 * col_width), "dp", scatter_dimension=1, tiled=True
    )
    rows_here = task_rows.shape[1]
    row_terms = jnp.dot(
        task_rows.reshape(NTASK * rows_here, 2 * col_width),
        pair_weight_t,
        precision=lax.Precision.HIGHEST,
    ).reshape(NTASK, rows_here, D)
    tile_grad = lax.psum_scatter(row_terms, "mp", scatter_dimension=2, tiled=True)
    source_grad, weight_part = tile_products(tile_grad, source_prompts, mix_weights, col_width)
    weight_grad = lax.psum(weight_part, ("dp", "mp"))
    logits_grad = mix_weights * (
        weight_grad - jnp.sum(mix_weights * weight_grad, axis=1, keepdims=True)
    )
    return (attended, source_grad, logits_grad)


BF = jnp.bfloat16
F32 = jnp.float32


def mm(a, b, ca=1, cb=0, precision=None):
    return lax.dot_general(
        a, b, (((ca,), (cb,)), ((), ())), preferred_element_type=F32, precision=precision
    )


def chain_kernel(
    ndp, nmp, nch,
    lg_hbm, ids_hbm, sp_hbm, kw_hbm, vw_hbm, q_hbm, k_hbm, v_hbm, c_hbm,
    att_hbm, tile_hbm, lg_out, w_hbm,
    logits, ids_in, tile_v, att_out, w_out, p_v, kw_v, vw_v, q_v, k_v, v_v, c_v,
    mixed, ids_own, ids_buf, tab, sbuf, pair, gr, rbuf, acc, ubuf, urec, ys, yr, zs, zr, zt, xr, wp, wbuf,
    lsem, gs, gv, fs, fv, js, jv, ts, tv, bs, bv, cs, cv, us, uv, hs, hv, es, ev, xv, ws, wv,
):
    n = ndp * nmp
    nz = nmp // 2
    ne = n // nz
    width = kw_v.shape[1]
    cw = width // nch
    rows = p_v.shape[1]
    nsrc = p_v.shape[0]
    ntask = logits.shape[0]
    tp = ntask * rows
    spn = nsrc * rows
    seq = q_v.shape[0]
    steps = nz * nch
    d = lax.axis_index("dp")
    m = lax.axis_index("mp")
    z = m // 2
    y = lax.rem(m, 2)
    me = d * nmp + m
    own = y * ndp + d
    up = 1 - 2 * (z // 2)
    inner = lax.rem((z + 1) // 2, 2)
    is_in = inner == 1
    nxt = z + up
    out_z = z - up * inner
    other = z * 2 + (1 - y)

    shift = rows.bit_length() - 1

    def iota(shape, axis):
        return lax.broadcasted_iota(jnp.int32, shape, axis)

    def outer(a):
        return lax.shift_right_logical(a, jnp.int32(shift))

    def same_row(shape):
        return ((iota(shape, 0) ^ iota(shape, 1)) & (rows - 1)) == 0

    def remote(src, dst, ss, rs, dd, mm_):
        return pltpu.make_async_remote_copy(
            src_ref=src, dst_ref=dst, send_sem=ss, recv_sem=rs,
            device_id=(dd, mm_), device_id_type=pl.DeviceIdType.MESH,
        )

    def drain(ref, sem):
        pltpu.make_async_copy(ref, ref, sem).wait()

    def place(i):
        i = jnp.int32(i)
        k = i // nch
        off_in = jnp.where(k == 2, -1, jnp.where(k == 3, 2, k))
        return z + up * (inner * off_in + (1 - inner) * k), lax.rem(i, nch)

    small = [
        pltpu.make_async_copy(lg_hbm, logits, lsem.at[9]),
        pltpu.make_async_copy(ids_hbm, ids_in, lsem.at[10]),
    ]
    for c in small:
        c.start()
    npl = 4
    loads = []
    for i in range(npl):
        s_at = pl.ds(i * (nsrc // npl), nsrc // npl)
        loads.append(
            pltpu.make_async_copy(
                sp_hbm.at[s_at, pl.ds(pl.multiple_of(d * rows, rows), rows), :],
                p_v.at[s_at], lsem.at[0],
            )
        )
        loads[i].start()
    for i, (a, b) in enumerate(
        ((kw_hbm, kw_v), (vw_hbm, vw_v), (k_hbm, k_v), (q_hbm, q_v), (v_hbm, v_v), (c_hbm, c_v))
    ):
        loads.append(pltpu.make_async_copy(a, b, lsem.at[1 + i]))

    def turn(i):
        i = jnp.int32(i)
        zz, h = place(i)
        late = z + up * lax.rem(i // nch + 1, nz)
        return jnp.where(is_in, zz, late), h

    barrier = pltpu.get_barrier_semaphore()

    @pl.loop(1, n)
    def _(k):
        to = lax.rem(me + k, n)
        pl.semaphore_signal(
            barrier, inc=1, device_id=(to // nmp, lax.rem(to, nmp)),
            device_id_type=pl.DeviceIdType.MESH,
        )

    for c in small:
        c.wait()
    lg = logits[...]
    ex = jnp.exp(lg - jnp.max(lg, axis=1, keepdims=True))
    mix = ex / jnp.sum(ex, axis=1, keepdims=True)
    upm = (
        outer(iota((tp, ntask), 0)) == iota((tp, ntask), 1)
    )
    tall = mm(jnp.where(upm, 1.0, 0.0), mix.astype(BF).astype(F32)).astype(BF)
    out = (
        outer(iota((nsrc, spn), 1)) == iota((nsrc, spn), 0)
    )
    wide = mm(tall, jnp.where(out, 1.0, 0.0).astype(BF))
    w_out[...] = jnp.where(same_row((tp, spn)), wide, 0.0).astype(BF)
    for j in range(ids_in.shape[0]):
        line = jnp.full((1, tp), ids_in[j], jnp.int32).astype(F32)
        ids_own[pl.ds(j, 1), :] = line
        ids_buf[d, pl.ds(j, 1), :] = line

    pltpu.make_async_copy(p_v, p_v, lsem.at[0]).wait()
    for c in loads[npl:]:
        c.start()
    w_save = pltpu.make_async_copy(w_out, w_hbm, lsem.at[7])
    w_save.start()
    for h in range(nch):
        mixed[m, h] = mm(w_out[...], p_v[:, :, pl.ds(h * cw, cw)].reshape(spn, cw)).astype(BF)

    pl.semaphore_wait(barrier, n - 1)

    def g_copy(zz, h, dz):
        slot = zz * 2 + y
        return remote(
            mixed.at[slot, h], mixed.at[slot, h], gs.at[0], gv.at[zz * nch + h], d, dz * 2 + y
        )

    def f_copy(zz, h, yy):
        slot = zz * 2 + yy
        return remote(
            mixed.at[slot, h], mixed.at[slot, h], fs.at[0], fv.at[zz * nch + h], d, other
        )

    for h in range(nch):
        f_copy(z, h, y).start()

        @pl.when(is_in)
        def _():
            g_copy(z, h, out_z).start()
            g_copy(z, h, nxt).start()

        @pl.when(jnp.logical_not(is_in))
        def _():
            g_copy(z, h, nxt).start()

    @pl.when(jnp.logical_not(is_in))
    def _():
        for h in range(nch):
            g_copy(z, h, z + 3 * up).start()

    for j in range(1, ndp):
        remote(ids_own, ids_buf.at[d], js.at[0], jv.at[0], lax.rem(d + j, ndp), m).start()
    loads[npl].wait()
    loads[npl + 1].wait()

    def part(slot, h):
        block = mixed[slot, h]
        at = pl.ds(pl.multiple_of(slot * width + h * cw, cw), cw)
        return mm(block, kw_v[at, :]), mm(block, vw_v[at, :])

    pk, pv = part(m, 0)
    for h in range(1, nch):
        a, b = part(m, h)
        pk, pv = pk + a, pv + b
    arrive = [(0, 0, h, h) for h in range(nch)]
    arrive += [(1, 1 - 2 * (i % 2), i, i // 2) for i in range(nch)]
    for i in range(2 * nch):
        k = nch + i
        side = (1 - 2 * (k % 2), k // 2) if k < 2 * nch else (2, k - 2 * nch)
        arrive.append((2 + i % 2, side[0], i // 2, side[1]))

    def arrival(i):
        off_o, off_i, h_o, h_i = arrive[i]
        return z + up * (off_o + inner * (off_i - off_o)), h_o + inner * (h_i - h_o)

    def from_z(i, pk, pv):
        zz, h = arrival(i)
        g_copy(zz, h, nxt).wait_recv()
        if arrive[i][1] != 2:
            @pl.when(is_in)
            def _():
                g_copy(zz, h, out_z if arrive[i][1] == 1 else nxt).start()

        f_copy(zz, h, y).start()
        a, b = part(zz * 2 + y, h)
        return pk + a, pv + b

    def from_y(i, pk, pv):
        zz, h = arrival(i)
        f_copy(zz, h, 1 - y).wait_recv()
        a, b = part(zz * 2 + (1 - y), h)
        return pk + a, pv + b

    lag = 2 * nch
    for i in range(nch, steps + lag):
        if i < steps:
            pk, pv = from_z(i, pk, pv)
        if i >= lag:
            pk, pv = from_y(i - lag, pk, pv)
    for h in range(nch):
        at = slice(h * cw, (h + 1) * cw)
        tab[z * nch + h, :, :cw] = pk[:, at].astype(BF)
        tab[z * nch + h, :, cw:] = pv[:, at].astype(BF)
        remote(
            tab.at[z * nch + h], tab.at[z * nch + h], ts.at[0], tv.at[z * nch + h],
            d, nxt * 2 + y,
        ).start()
    drain(ids_buf.at[pl.ds(0, ndp - 1)], jv.at[0])

    ids_all = ids_buf[...].reshape(n, tp).astype(BF)
    q_rows = 2 * ne * rows
    q = outer(iota((q_rows, n), 0))
    q_z = jnp.where(q < ne, z, out_z)
    q_in = q & (ne - 1)
    q_dev = lax.rem(q_in, jnp.int32(ndp)) * nmp + q_z * 2 + q_in // jnp.int32(ndp)
    ids_x = mm(jnp.where(q_dev == iota((q_rows, n), 1), 1.0, 0.0).astype(BF), ids_all)
    sel = jnp.where(
        (ids_x == outer(iota((q_rows, tp), 1)).astype(F32)) & same_row((q_rows, tp)), 1.0, 0.0
    ).astype(BF)
    sel_own = sel[: ne * rows]

    def row_at(dd):
        return pl.ds(pl.multiple_of(dd * rows, rows), rows)

    def col_at(zz, yy, h):
        return pl.ds(pl.multiple_of((zz * 2 + yy) * width + h * cw, cw), cw)

    def t_copy(zz, h, dz):
        k = zz * nch + h
        return remote(tab.at[k], tab.at[k], ts.at[0], tv.at[k], d, dz * 2 + y)

    def b_copy(zz, h, e, to_out):
        k = zz * nch + h
        g = e + to_out * ne
        return remote(
            sbuf.at[k * 2 * ne + g], pair.at[:, row_at(d), col_at(zz, y, h)],
            bs.at[0], bv.at[k],
            lax.rem(e, ndp), (out_z if to_out else z) * 2 + e // ndp,
        )

    def relay(i):
        zz, h = place(i)
        k = zz * nch + h

        @pl.when(zz != z)
        def _():
            t_copy(zz, h, nxt).wait_recv()

        @pl.when(is_in & (zz == out_z))
        def _():
            t_copy(zz, h, nxt).start()

        got = mm(sel, tab[k]).astype(BF)
        to = pl.ds(k * 2 * ne, 2 * ne)
        sbuf[to, 0] = got[:, :cw].reshape(2 * ne, rows, cw)
        sbuf[to, 1] = got[:, cw:].reshape(2 * ne, rows, cw)

        @pl.loop(1, ne)
        def _(r):
            b_copy(zz, h, lax.rem(own + r, ne), 0).start()

        pair[:, row_at(d), col_at(zz, y, h)] = sbuf[k * 2 * ne + own]

    def outward(i, first, count):
        zz, h = place(i)

        @pl.when(zz != out_z)
        def _():
            @pl.loop(first, first + count)
            def _(r):
                b_copy(zz, h, lax.rem(y * ndp + r, ne), 1).start()

    for i in range(nch):
        relay(i)

    @pl.when(is_in)
    def _():
        for side in range(2):
            for i in range(nch):
                outward(i, side * ndp, ndp)

    for c in loads[npl + 2:]:
        c.wait()

    def c_copy(zz, h, e):
        k = zz * nch + h
        return remote(
            gr.at[:, row_at(lax.rem(e, ndp)), col_at(zz, e // ndp, h)], rbuf.at[k * ne + own],
            cs.at[0], cv.at[k], lax.rem(e, ndp), z * 2 + e // ndp,
        )

    scale = DH ** (-0.5)
    to_exp2 = scale * 1.4426950408889634
    ptok = pair.shape[1]
    seen = iota((seq, seq), 0) <= iota((seq, seq), 1)

    def group(i):
        zz, h = turn(i)

        @pl.when(is_in | (zz == z))
        def _():
            drain(rbuf.at[pl.ds(0, ne - 1)], bv.at[zz * nch + h])

        @pl.when(jnp.logical_not(is_in | (zz == z)))
        def _():
            drain(rbuf.at[pl.ds(0, ne)], bv.at[zz * nch + h])

        ats, st, gt, va = [], [], [], []
        for yy in range(2):
            for hh in range(cw // DH):
                base = (zz * 2 + yy) * width + h * cw + hh * DH
                at = pl.ds(pl.multiple_of(base, DH), DH)
                ats.append(at)
                ka = jnp.concatenate([pair[0, :, at], k_v[:, at]], axis=0)
                va.append(jnp.concatenate([pair[1, :, at], v_v[:, at]], axis=0))
                st.append(mm(ka, q_v[:, at], 1, 1))
                gt.append(mm(va[-1], c_v[:, at], 1, 1))
        for j, at in enumerate(ats):
            s = st[j] * to_exp2
            s = jnp.concatenate([s[:ptok], jnp.where(seen, s[ptok:], mask_fill)], axis=0)
            e = jnp.exp2(s - jnp.max(s, axis=0, keepdims=True))
            a = e * (1.0 / jnp.sum(e, axis=0, keepdims=True))
            ab = a.astype(BF)
            inner_sum = jnp.sum(a * gt[j], axis=0, keepdims=True)
            gs1 = (a[:ptok] * (gt[j][:ptok] - inner_sum)).astype(BF)
            gr[0, :, at] = (mm(gs1, q_v[:, at]) * scale).astype(BF)
            gr[1, :, at] = mm(ab[:ptok], c_v[:, at]).astype(BF)
            att_out[:, at] = mm(ab, va[j], 0, 0).astype(BF)

        @pl.loop(1, ne)
        def _(r):
            c_copy(zz, h, lax.rem(own + r, ne)).start()

        rbuf[(zz * nch + h) * ne + own] = gr[:, row_at(d), col_at(zz, y, h)]

    def u_copy(zz, h, dz, slot):
        k = zz * nch + h
        return remote(
            ubuf.at[k], urec.at[slot * nch + h], us.at[0], uv.at[slot * nch + h], d, dz * 2 + y
        )

    def total(i):
        zz, h = turn(i)
        k = zz * nch + h

        drain(rbuf.at[pl.ds(0, ne - 1)], cv.at[k])
        at = pl.ds(k * ne, ne)
        acc[k, :, :cw] = mm(sel_own, rbuf[at, 0].reshape(ne * rows, cw), 0, 0)
        acc[k, :, cw:] = mm(sel_own, rbuf[at, 1].reshape(ne * rows, cw), 0, 0)

        @pl.when(is_in & (zz == out_z))
        def _():
            ubuf[k] = acc[k].astype(BF)
            u_copy(zz, h, zz, z).start()

        @pl.when(jnp.logical_not(is_in | (zz == z)))
        def _():
            ubuf[k] = acc[k].astype(BF)
            u_copy(zz, h, nxt, zz).start()

    def combine(i):
        zz, h = turn(i)
        k = zz * nch + h
        u_copy(zz, h, nxt, zz).wait_recv()
        ubuf[k] = (acc[k] + urec[k].astype(F32)).astype(BF)
        u_copy(zz, h, zz, jnp.where(zz == nxt, z + 2 * up, z)).start()

    ahead = 2 * nch

    @pl.when(is_in)
    def _():
        @pl.loop(nch, ahead)
        def _(i):
            relay(i)
            outward(i, 0, ne)

    @pl.loop(0, steps)
    def _(i):
        group(i)

        @pl.when(is_in & (i < steps - ahead))
        def _():
            relay(i + ahead)
            outward(i + ahead, 0, ne)

        @pl.when(i >= nch)
        def _():
            total(i - nch)

        @pl.when(is_in & (i >= 3 * nch))
        def _():
            combine(i - 2 * nch)

    att_save = pltpu.make_async_copy(att_out, att_hbm, lsem.at[8])
    att_save.start()

    @pl.loop(steps - nch, steps)
    def _(i):
        total(i)

    @pl.when(is_in)
    def _():
        @pl.loop(steps - nch, steps)
        def _(i):
            combine(i)

    s1 = z + up * (1 - inner)
    s2 = z + up * (2 - 3 * inner)
    tks, tvs = [], []
    for h in range(nch):
        u_copy(z, h, nxt, s1).wait_recv()
        u_copy(z, h, nxt, s2).wait_recv()
        k = z * nch + h
        acc[k] = acc[k] + urec[s1 * nch + h].astype(F32) + urec[s2 * nch + h].astype(F32)

        t = acc[k].astype(BF)
        tks.append(t[:, :cw])
        tvs.append(t[:, cw:])
    tk = jnp.concatenate(tks, axis=1)
    tv_ = jnp.concatenate(tvs, axis=1)

    def term(slot):
        at = pl.ds(pl.multiple_of(slot * width, width), width)
        return mm(tk, kw_v[at, :], 1, 1) + mm(tv_, vw_v[at, :], 1, 1)

    def target(j):
        return z + up * ((nz - 1 - j) * (1 - inner) + inner * (2, 1, -1, 0)[j])

    def y_copy(j, h):
        k = j * nch + h
        return remote(ys.at[k], yr.at[k], hs.at[0], hv.at[k], d, other)

    def z_copy(zz, h, dz, slot):
        k = zz * nch + h
        return remote(
            zs.at[k], zr.at[slot * nch + h], es.at[0], ev.at[slot * nch + h], d, dz * 2 + y
        )

    def cut(a, h):
        return a[:, h * cw : (h + 1) * cw]

    def x_copy(h):
        k = 2 * nch + h
        return remote(ys.at[k], xr.at[h], hs.at[0], xv.at[h], d, nxt * 2 + y)

    for j in (0, 2, 1, 3):
        got = term(target(j) * 2 + (1 - y))
        if j == 3:
            zt[j] = got
        for h in range(nch):
            if j < 3:
                ys[j * nch + h] = cut(got, h).astype(BF)
            if j == 2:
                @pl.when(is_in)
                def _():
                    y_copy(j, h).start()

                @pl.when(jnp.logical_not(is_in))
                def _():
                    x_copy(h).start()
            elif j < 2:
                y_copy(j, h).start()

    @pl.when(jnp.logical_not(is_in))
    def _():
        for h in range(nch):
            ys[3 * nch + h] = zt[3, :, h * cw : (h + 1) * cw].astype(BF)
            y_copy(3, h).start()
        got = term(nxt * 2 + y)
        for h in range(nch):
            zs[nxt * nch + h] = cut(got, h).astype(BF)

    for j in (0, 1):
        zt[j] = term(target(j) * 2 + y)

    @pl.when(is_in)
    def _():
        got = term(out_z * 2 + y)
        for h in range(nch):
            k = out_z * nch + h
            y_copy(2, h).wait_recv()
            zs[k] = (cut(got, h) + yr[2 * nch + h].astype(F32)).astype(BF)
            z_copy(out_z, h, out_z, z).start()
        for h in range(nch):
            x_copy(h).wait_recv()
            k = 3 * nch + h
            ys[k] = (zt[3, :, h * cw : (h + 1) * cw] + xr[h].astype(F32)).astype(BF)
            y_copy(3, h).start()

    zt[3] = term(z * 2 + y)

    def route(j):
        zz = target(j)
        if j == 0:
            return jnp.where(is_in, zz, nxt), jnp.where(is_in, z, zz)
        return jnp.where(is_in, zz, nxt), jnp.where(is_in, z + 2 * up, zz)

    tile, sums = [], []
    for j in (0, 1, 3):
        zz = target(j)
        if j == 3:
            @pl.when(jnp.logical_not(is_in))
            def _():
                for h in range(nch):
                    z_copy(nxt, h, nxt, nxt).start()

        for h in range(nch):
            k = zz * nch + h
            y_copy(j, h).wait_recv()
            mine = zt[j, :, h * cw : (h + 1) * cw] + yr[j * nch + h].astype(F32)
            if j == nz - 1:
                z_copy(z, h, nxt, s1).wait_recv()
                z_copy(z, h, nxt, s2).wait_recv()
                mine = mine + zr[s1 * nch + h].astype(F32) + zr[s2 * nch + h].astype(F32)
                piece = mine.astype(BF)
                tile.append(piece)
                half = p_v[:, :, h * cw : (h + 1) * cw].reshape(spn, cw)
                got = jnp.where(same_row((spn, tp)), mm(half, piece, 1, 1), 0.0)
                sums.append(jnp.sum(got.reshape(nsrc, rows, tp), axis=1))
                continue
            acc[k, :, :cw] = mine

            @pl.when(is_in)
            def _():
                z_copy(zz, h, zz, zz).wait_recv()
                acc[k, :, :cw] = acc[k, :, :cw] + zr[k].astype(F32)

            zs[k] = acc[k, :, :cw].astype(BF)
            dz, slot = route(j)
            z_copy(zz, h, dz, slot).start()
    tile = jnp.concatenate(tile, axis=1)
    tile_v[...] = tile
    tile_save = pltpu.make_async_copy(tile_v, tile_hbm, lsem.at[11])
    tile_save.start()

    prod = sum(sums[1:], sums[0])
    fold = (
        outer(iota((ntask, tp), 1)) == iota((ntask, tp), 0)
    )
    part_w = mm(jnp.where(fold, 1.0, 0.0), prod, 1, 1, lax.Precision.HIGHEST)
    wp[...] = part_w
    wbuf[me] = part_w

    def w_copy(k):
        to = lax.rem(me + k, n)
        return remote(wp, wbuf.at[me], ws.at[0], wv.at[0], to // nmp, lax.rem(to, nmp))

    @pl.loop(1, n)
    def _(k):
        w_copy(k).start()

    w_save.wait()
    att_save.wait()
    tile_save.wait()

    moved = steps - nch
    drain(mixed.at[pl.ds(0, nz)], fs.at[0])
    drain(ids_buf.at[pl.ds(0, ndp - 1)], js.at[0])
    drain(rbuf.at[pl.ds(0, steps * (ne - 1))], cs.at[0])
    drain(ubuf.at[pl.ds(0, moved)], us.at[0])
    drain(ys, hs.at[0])
    drain(zs.at[pl.ds(0, moved)], es.at[0])

    @pl.when(is_in)
    def _():
        drain(mixed.at[pl.ds(0, nz)], gs.at[0])
        drain(tab.at[pl.ds(0, 2 * nch)], ts.at[0])
        drain(sbuf.at[pl.ds(0, steps * (ne - 1) + moved * ne)], bs.at[0])

    @pl.when(jnp.logical_not(is_in))
    def _():
        drain(mixed.at[pl.ds(0, nz // 2)], gs.at[0])
        drain(tab.at[pl.ds(0, nch)], ts.at[0])
        drain(sbuf.at[pl.ds(0, nch * (ne - 1))], bs.at[0])

    drain(wbuf.at[pl.ds(0, n - 1)], ws.at[0])
    drain(wbuf.at[pl.ds(0, n - 1)], wv.at[0])

    wg = jnp.sum(wbuf[...], axis=0)
    lg_out[...] = mix * (wg - jnp.sum(mix * wg, axis=1, keepdims=True))


def source_kernel(
    parts, w_hbm, tile_hbm, att_hbm, lg_hbm, out_hbm, att_out, lg_out,
    w_v, tile_v, att_v, lg_v, out_v, isem, osem,
):
    nsrc, rows, width = out_hbm.shape
    cols = nsrc * rows // parts
    part = nsrc // parts
    tile_in = pltpu.make_async_copy(tile_hbm, tile_v, isem.at[parts])
    tile_in.start()
    ins, outs = [], []
    for i in range(parts):
        at = pl.ds(i * cols, cols)
        ins.append(pltpu.make_async_copy(w_hbm.at[:, at], w_v.at[:, at], isem.at[i]))
        ins[i].start()
    att_in = pltpu.make_async_copy(att_hbm, att_v, isem.at[parts + 1])
    lg_in = pltpu.make_async_copy(lg_hbm, lg_v, isem.at[parts + 2])
    att_in.start()
    lg_in.start()
    tile_in.wait()
    for i in range(parts):
        ins[i].wait()
        at = pl.ds(i * part, part)
        got = mm(w_v[:, i * cols : (i + 1) * cols], tile_v[...], 0, 0)
        out_v[at] = got.reshape(part, rows, width)
        outs.append(pltpu.make_async_copy(out_v.at[at], out_hbm.at[at], osem.at[i]))
        outs[i].start()
        if i == 0:
            att_in.wait()
            outs_att = pltpu.make_async_copy(att_v, att_out, osem.at[parts])
            outs_att.start()
            lg_in.wait()
            outs_lg = pltpu.make_async_copy(lg_v, lg_out, osem.at[parts + 1])
            outs_lg.start()
    for c in outs + [outs_att, outs_lg]:
        c.wait()


def per_device(ndp, nmp, *args):
    source_prompts, task_logits, task_ids, key_weight, value_weight = args[:5]
    queries, keys, values, cotangent = args[5:]
    nsrc, ptok, width = source_prompts.shape
    ntask = task_logits.shape[0]
    ge = task_ids.shape[0]
    rows = ptok // ndp
    nch = 2
    if width % (nch * DH) or nmp != 8 or ndp & (ndp - 1) or ge != nmp or ptok % ndp or rows % 16 or rows & (rows - 1) or ntask * rows != 128:
        return on_device(*args)
    n, nz = ndp * nmp, nmp // 2
    ne, st, cw = n // nz, nz * nch, width // nch
    tp, spn = ntask * rows, nsrc * rows
    seq, full = queries.shape[1:]
    vmem = pl.BlockSpec(memory_space=pltpu.VMEM)
    hbm = pl.BlockSpec(memory_space=pl.ANY)
    dma = pltpu.SemaphoreType.DMA
    attended, tile, logits_grad, w_big = pl.pallas_call(
        functools.partial(chain_kernel, ndp, nmp, nch),
        out_shape=(
            jax.ShapeDtypeStruct((seq, full), BF),
            jax.ShapeDtypeStruct((tp, width), BF),
            jax.ShapeDtypeStruct((ntask, nsrc), F32),
            jax.ShapeDtypeStruct((tp, spn), BF),
        ),
        in_specs=[hbm] * 9,
        out_specs=(hbm, hbm, vmem, hbm),
        scratch_shapes=[
            pltpu.VMEM((ntask, nsrc), F32),
            pltpu.SMEM((ge,), jnp.int32),
            pltpu.VMEM((tp, width), BF),
            pltpu.VMEM((seq, full), BF),
            pltpu.VMEM((tp, spn), BF),
            pltpu.VMEM((nsrc, rows, width), BF),
            pltpu.VMEM((full, width), BF),
            pltpu.VMEM((full, width), BF),
            pltpu.VMEM((seq, full), BF),
            pltpu.VMEM((seq, full), BF),
            pltpu.VMEM((seq, full), BF),
            pltpu.VMEM((seq, full), BF),
            pltpu.VMEM((nmp, nch, tp, cw), BF),
            pltpu.VMEM((ge, tp), F32),
            pltpu.VMEM((ndp, ge, tp), F32),
            pltpu.VMEM((st, tp, 2 * cw), BF),
            pltpu.VMEM((st * 2 * ne, 2, rows, cw), BF),
            pltpu.VMEM((2, ptok, full), BF),
            pltpu.VMEM((2, ptok, full), BF),
            pltpu.VMEM((st * ne, 2, rows, cw), BF),
            pltpu.VMEM((st, tp, 2 * cw), F32),
            pltpu.VMEM((st, tp, 2 * cw), BF),
            pltpu.VMEM((st, tp, 2 * cw), BF),
            pltpu.VMEM((st, tp, cw), BF),
            pltpu.VMEM((st, tp, cw), BF),
            pltpu.VMEM((st, tp, cw), BF),
            pltpu.VMEM((st, tp, cw), BF),
            pltpu.VMEM((nz, tp, width), F32),
            pltpu.VMEM((nch, tp, cw), BF),
            pltpu.VMEM((ntask, nsrc), F32),
            pltpu.VMEM((n, ntask, nsrc), F32),
            dma((12,)),
            dma((1,)), dma((st,)), dma((1,)), dma((st,)), dma((1,)), dma((1,)),
            dma((1,)), dma((st,)), dma((1,)), dma((st,)), dma((1,)), dma((st,)),
            dma((1,)), dma((st,)), dma((1,)), dma((st,)), dma((1,)), dma((st,)),
            dma((nch,)), dma((1,)), dma((1,)),
        ],
        compiler_params=pltpu.CompilerParams(
            collective_id=0, has_side_effects=True, vmem_limit_bytes=60 * 2**20
        ),
        name="chain",
    )(
        task_logits, task_ids, source_prompts, key_weight, value_weight,
        queries.reshape(seq, full), keys.reshape(seq, full),
        values.reshape(seq, full), cotangent.reshape(seq, full),
    )
    parts = 4
    source_grad, attended, logits_grad = pl.pallas_call(
        functools.partial(source_kernel, parts),
        out_shape=(
            jax.ShapeDtypeStruct((nsrc, rows, width), F32),
            jax.ShapeDtypeStruct((seq, full), BF),
            jax.ShapeDtypeStruct((ntask, nsrc), F32),
        ),
        in_specs=[hbm] * 4,
        out_specs=(hbm, hbm, hbm),
        scratch_shapes=[
            pltpu.VMEM((tp, spn), BF),
            pltpu.VMEM((tp, width), BF),
            pltpu.VMEM((seq, full), BF),
            pltpu.VMEM((ntask, nsrc), F32),
            pltpu.VMEM((nsrc, rows, width), F32),
            dma((parts + 3,)), dma((parts + 2,)),
        ],
        compiler_params=pltpu.CompilerParams(vmem_limit_bytes=60 * 2**20),
        name="source_grad",
    )(w_big, tile, attended, logits_grad)
    return (attended.reshape(queries.shape), source_grad, logits_grad)


def solution(mesh):
    placed = (
        P(None, None, "mp"),
        P(),
        P("dp"),
        P(None, "mp"),
        P(None, "mp"),
        P(("dp", "mp"), None, None),
        P(("dp", "mp"), None, None),
        P(("dp", "mp"), None, None),
        P(("dp", "mp"), None, None),
    )
    return jax.shard_map(
        functools.partial(per_device, mesh.shape["dp"], mesh.shape["mp"]),
        mesh=mesh,
        in_specs=placed,
        out_specs=(P(("dp", "mp"), None, None), P(None, "dp", "mp"), P()),
        check_vma=False,
    )
```
